8 devices in a mesh: dp: 2 (over y, z), sp: 4 (over x, core).
Axes of the slice: x: 2, y: 2, z: 1, core: 2. Of those that a mesh axis runs over, the one named last changes fastest.
Arguments:
- x: bfloat16 [4096, 2048], P(('dp', 'sp')), parts along dimension 0
- gain: bfloat16 [2048], replicated
- wq: bfloat16 [2048, 4096], replicated
- wk: bfloat16 [2048, 2048], replicated
- wv: bfloat16 [2048, 2048], replicated
- wo: bfloat16 [4096, 2048], replicated
Outputs:
- output: bfloat16 [4096, 2048], P(('dp', 'sp')), parts along dimension 0
There are 2 independent parts. The reference program is written for one: setup_inputs(seed, part) draws one part's arguments, and reference() takes and returns one part's arrays. A program takes and returns all parts, laid end to end along the dimension named above; an argument that names none is the same for every part.
All inputs are finite; a program needn't handle non-finite values.
Results may differ from the reference program's by a relative error of at most 0.012.
Values are sent between devices in bfloat16 or wider.
A program may use at most 2 GiB of HBM per device.

```python
import jax
import jax.numpy as jnp
from jax import lax

ROWS = 2048
D = 2048
HEADS = 32
KV_HEADS = 16
HEAD = 128
THETA = 10000


def setup_inputs(seed: int = 0, part: int = 0) -> dict:
    kx, kn, kq, kk, kv, ko = jax.random.split(jax.random.key(seed), 6)

    def weights(key, rows, columns):
        return jax.random.normal(key, (rows, columns), jnp.float32) * rows**-0.5

    drawn = {
        "x": jax.random.normal(jax.random.fold_in(kx, part), (ROWS, D), jnp.float32),
        "gain": 1 + 0.1 * jax.random.normal(kn, (D,), jnp.float32),
        "wq": 2 * weights(kq, D, HEADS * HEAD),
        "wk": 2 * weights(kk, D, KV_HEADS * HEAD),
        "wv": 4 * weights(kv, D, KV_HEADS * HEAD),
        "wo": weights(ko, HEADS * HEAD, D),
    }
    return {k: v.astype(jnp.bfloat16) for k, v in drawn.items()}


def normed(x, gain):
    wide = x.astype(jnp.float32)
    scale = lax.rsqrt(jnp.mean(wide * wide, -1, keepdims=True) + 1e-6)
    return (wide * scale * gain.astype(jnp.float32)).astype(jnp.bfloat16)


def turned(t, place, theta):
    half = t.shape[-1] // 2
    angle = place.astype(jnp.float32)[:, None] * theta ** (-jnp.arange(half, dtype=jnp.float32) / half)
    cos, sin = jnp.cos(angle)[:, None], jnp.sin(angle)[:, None]
    a, b = t[..., :half].astype(jnp.float32), t[..., half:].astype(jnp.float32)
    return jnp.concatenate([a * cos - b * sin, b * cos + a * sin], -1).astype(jnp.bfloat16)


def matmul(a, w):
    return jnp.dot(a, w, preferred_element_type=jnp.float32).astype(jnp.bfloat16)


def einsum(form, a, b):
    return jnp.einsum(form, a.astype(jnp.float32), b.astype(jnp.float32))


def attention(q, k, v):
    scores = einsum("tgsd,ugd->gstu", q, k) * q.shape[-1] ** -0.5
    token = jnp.arange(q.shape[0])
    scores = jnp.where(token[:, None] >= token, scores, -jnp.inf)
    weights = jax.nn.softmax(scores, -1).astype(jnp.bfloat16)
    return einsum("gstu,ugd->tgsd", weights, v).astype(jnp.bfloat16)


def reference(x, gain, wq, wk, wv, wo):
    a, place = normed(x, gain), jnp.arange(ROWS)
    q = turned(matmul(a, wq).reshape(ROWS, HEADS, HEAD), place, THETA).reshape(ROWS, KV_HEADS, -1, HEAD)
    k = turned(matmul(a, wk).reshape(ROWS, KV_HEADS, HEAD), place, THETA)
    v = matmul(a, wv).reshape(ROWS, KV_HEADS, HEAD)
    seen = attention(q, k, v).reshape(ROWS, HEADS * HEAD)
    return (x.astype(jnp.float32) + jnp.dot(seen, wo, preferred_element_type=jnp.float32)).astype(jnp.bfloat16)
```

```python
import functools

import jax
import jax.numpy as jnp
import numpy as np
from jax import lax
from jax.experimental import pallas as pl
from jax.experimental.pallas import tpu as pltpu
from jax.sharding import PartitionSpec as P

HEAD = 128
THETA = 10000
NEG = -1e30
HIDDEN = 2 * NEG
LOG2E = 1.4426950408889634
E = HEAD**-0.5 * LOG2E
D = 2048
KVH = 8
GRP = 4
BQ = 256
COLS = 2 * BQ
OWN = 512
TM = 256
MESH = pl.DeviceIdType.MESH


def _dot(a, b, ca, cb):
    return lax.dot_general(a, b, (((ca,), (cb,)), ((), ())), preferred_element_type=jnp.float32)


def _al(v, n):
    return pl.multiple_of(v, n)


def _kernel(x_ref, gain_ref, hi_ref, lo_ref, wq_ref, wk_ref, wv_ref, wo_ref, y_ref,
            xs, ab, wkv, wqo, kb, vt, qo, ox, top, mix, loc, snd, rcv):
    me = lax.axis_index("sp")
    ci, cc = lax.div(me, 2), lax.rem(me, 2)
    par = 2 * ci + 1 - cc
    far = 2 * (1 - ci) + cc

    def local(src, dst, i):
        return pltpu.make_async_copy(src, dst, loc.at[i])

    def remote(src, dst, i, to, s=None):
        return pltpu.make_async_remote_copy(src_ref=src, dst_ref=dst, send_sem=snd.at[i if s is None else s], recv_sem=rcv.at[i],
                                            device_id={"sp": to}, device_id_type=MESH)

    get_x = local(x_ref, xs.at[pl.ds(0, OWN)], 0)
    get_wk = local(wk_ref.at[:, pl.ds(_al(cc * 1024, 1024), 1024)], wkv.at[:, pl.ds(0, 1024)], 1)
    get_wv = local(wv_ref.at[:, pl.ds(_al(cc * 1024, 1024), 1024)], wkv.at[:, pl.ds(1024, 1024)], 2)
    get_wq = local(wq_ref.at[:, pl.ds(_al(cc * D, D), D)], wqo, 3)
    get_wo = local(wo_ref.at[pl.ds(_al(cc * D, D), D)], wqo, 4)
    get_wo2 = local(wo_ref.at[pl.ds(_al((1 - cc) * D, D), D)], wkv, 5)
    get_x.start()
    get_wk.start()
    get_wv.start()
    get_wq.start()

    barrier = pltpu.get_barrier_semaphore()
    for k in range(1, 4):
        pl.semaphore_signal(barrier, inc=1, device_id={"sp": lax.rem(me + k, 4)}, device_id_type=MESH)
    pl.semaphore_wait(barrier, 3)

    mine = _al(me * OWN, OWN)
    theirs = _al(par * OWN, OWN)
    send_a = remote(ab.at[pl.ds(mine, OWN)], ab.at[pl.ds(mine, OWN)], 0, par)

    def send_far(h):
        at = pl.ds(_al(cc * OWN + h * 256, 256), 256)
        return remote(ab.at[at], ab.at[at], 1 + h, far)

    def relay(h):
        at = pl.ds(_al(cc * OWN + h * 256, 256), 256)
        return remote(ab.at[at], ab.at[at], 3 + h, par)

    def send_xt(k):
        return remote(x_ref.at[pl.ds(128 * k, 128)], xs.at[pl.ds(OWN, 128)], 5, k, 5 + k)

    at_t = pl.ds(_al(1024 + cc * 128, 128), 128)
    send_at = remote(ab.at[at_t], ab.at[at_t], 7, par)

    def send_o(src, rows, dst, i):
        return remote(qo.at[pl.ds(src, rows)], ox.at[pl.ds(dst, rows)], i, par)

    def send_yt(c):
        return remote(xs.at[pl.ds(OWN, 128)], y_ref.at[pl.ds(128 * c, 128)], 13 + c, 2)

    @pl.when(me == 2)
    def _():
        send_xt(0).start()
        send_xt(1).start()

    def norm(src, dst, rows):
        def some(j, _):
            wide = xs[pl.ds(_al(src + 32 * j, 32), 32), :].astype(jnp.float32)
            scale = lax.rsqrt(jnp.mean(wide * wide, -1, keepdims=True) + 1e-6)
            ab[pl.ds(_al(dst + 32 * j, 32), 32), :] = (wide * scale * gain_ref[...].astype(jnp.float32)).astype(jnp.bfloat16)
        lax.fori_loop(0, rows // 32, some, None)

    get_x.wait()
    norm(0, mine, OWN)
    send_a.start()

    @pl.when(ci == 0)
    def _():
        send_far(0).start()
        send_far(1).start()

    for h in range(KVH):
        vt[h, HEAD:, :] = jnp.ones((16, D), jnp.bfloat16)

    def angles(r):
        cl, sl = lo_ref[:128, :], lo_ref[128:, :]
        cs, ss = [], []
        for k in range(2):
            n = lax.div(r, 128) + k
            ch, sh = hi_ref[pl.ds(n, 1), :], hi_ref[pl.ds(16 + n, 1), :]
            cs.append(ch * cl - sh * sl)
            ss.append(sh * cl + ch * sl)
        return jnp.concatenate(cs, 0), jnp.concatenate(ss, 0)

    def turned(t, cos, sin):
        t = t.astype(jnp.bfloat16).astype(jnp.float32)
        return (t * cos + pltpu.roll(t, 64, 1) * sin).astype(jnp.bfloat16)

    def kv_step(r, pos):
        cos, sin = angles(r)
        for n in range(4):
            t = _dot(ab[pl.ds(r, 256), :], wkv[:, 256 * n : 256 * n + 256], 1, 0)
            for k in range(2):
                kb[2 * n + k, pl.ds(pos, 256), :] = turned(t[:, 128 * k : 128 * k + 128], cos, sin)
        for n in range(4):
            t = _dot(ab[pl.ds(r, 256), :], wkv[:, 1024 + 256 * n : 1024 + 256 * n + 256], 1, 0).astype(jnp.bfloat16)
            for k in range(2):
                vt[2 * n + k, :HEAD, pl.ds(pos, 256)] = t[:, 128 * k : 128 * k + 128].T

    def q_step(r, pos):
        cos, sin = angles(r)
        for n in range(8):
            t = _dot(ab[pl.ds(r, 256), :], wqo[:, 256 * n : 256 * n + 256], 1, 0)
            for k in range(2):
                qo[pl.ds(pos, 256), 256 * n + 128 * k : 256 * n + 128 * k + 128] = turned(t[:, 128 * k : 128 * k + 128], cos, sin)

    def attend(qs, slot, kp, full, small, level, begin, end):
        def group(g, _):
            h0 = g * GRP

            def q_of(i):
                a = [qo[pl.ds(qs, BQ), pl.ds(_al((h0 + i) * 256 + 128 * n, 128), 128)] for n in range(2)]
                return jnp.concatenate(a, 0)

            @pl.when(begin)
            def _():
                for i in range(GRP):
                    top[slot, h0 + i] = jnp.full((1, COLS), NEG, jnp.float32)
                    mix[slot, h0 + i] = jnp.zeros((HEAD + 8, COLS), jnp.float32)

            def block(at, bk, level):
                scores = [_dot(kb[h0 + i, pl.ds(at, bk), :], q_of(i), 1, 1) for i in range(GRP)]
                if level is not None:
                    gap = lax.rem(lax.broadcasted_iota(jnp.int32, (bk, COLS), 1), BQ) - lax.broadcasted_iota(jnp.int32, (bk, COLS), 0)
                    ok = gap >= level
                weights, keeps = [], []
                for i, s in enumerate(scores):
                    if level is not None:
                        s = jnp.where(ok, s, HIDDEN)
                    old = top[slot, h0 + i]
                    new = jnp.maximum(old, s.max(axis=0, keepdims=True))
                    top[slot, h0 + i] = new
                    weights.append(jnp.exp2((s - new) * E).astype(jnp.bfloat16))
                    keeps.append(jnp.exp2((old - new) * E))
                for i, (p, keep) in enumerate(zip(weights, keeps)):
                    add = _dot(vt[h0 + i, :, pl.ds(at, bk)], p, 1, 0)
                    mix[slot, h0 + i] = mix[slot, h0 + i] * keep + add[: HEAD + 8]

            lax.fori_loop(0, full, lambda j, _: block(_al(kp + 512 * j, 256), 512, None), None)
            kq = kp + 512 * full
            lax.fori_loop(0, small, lambda j, _: block(_al(kq + 256 * j, 256), 256, level + 256 * j), None)

            @pl.when(end)
            def _():
                for i in range(GRP):
                    total = mix[slot, h0 + i, HEAD : HEAD + 1, :]
                    out = (mix[slot, h0 + i, :HEAD, :] * (1 / total)).T.astype(jnp.bfloat16)
                    for n in range(2):
                        qo[pl.ds(qs, BQ), pl.ds(_al((h0 + i) * 256 + 128 * n, 128), 128)] = out[BQ * n : BQ * n + BQ]

        lax.fori_loop(0, KVH // GRP, group, None)

    def phase(p, _):
        late = (ci == 1) & (p >= 1)

        @pl.when(late)
        def _():
            send_far(p - 1).wait_recv()
            relay(p - 1).start()

        def kv(j, _):
            @pl.when((p == 0) & (j == 0))
            def _():
                get_wk.wait()
                get_wv.wait()

            @pl.when((p == 0) & (j == 2))
            def _():
                send_a.wait_recv()

            @pl.when((p == 1) & (ci == 0))
            def _():
                send_at.wait_recv()

            @pl.when(late & (j == 1))
            def _():
                relay(p - 1).wait_recv()

            first = jnp.where(p == 0, 1, 0)
            jj, jh = lax.rem(j, 2), lax.div(j, 2)
            r0 = jnp.where(jh == 0, me, par) * OWN + 256 * jj
            r1 = jnp.where(ci == 0, 1024, jnp.where(j == 0, cc, 1 - cc) * OWN + 256 * (p - 1))
            r = jnp.where(first == 1, r0, r1)
            pos = jnp.where((first == 1) | (ci == 0), r, 512 * (p - 1) + 256 * j)
            kv_step(_al(r, 256), _al(pos, 256))

        n_kv = jnp.where(p == 0, 4, jnp.where(ci == 1, 2, jnp.where(p == 1, 1, 0)))
        lax.fori_loop(0, n_kv, kv, None)

        @pl.when(p == 1 + ci)
        def _():
            get_wo2.start()

        def q(j, _):
            @pl.when((p == 0) & (j == 0))
            def _():
                get_wq.wait()

            @pl.when((p == 0) & (ci == 0) & (j == 2))
            def _():
                send_xt(0).wait_recv()
                norm(OWN, 1024 + cc * 128, 128)
                send_at.start()

            pos = jnp.where(p == 0, 256 * j, 1024)
            q_step(_al(pos + 1280 * ci, 256), _al(pos, 256))

        n_q = jnp.where(p == 0, 4 - ci, jnp.where((p == 1) & (ci == 0), 1, 0))
        lax.fori_loop(0, n_q, q, None)

        @pl.when(p == 1 - ci)
        def _():
            get_wo.start()

        def att(it, _):
            b = lax.rem(it + 1 - cc, 3)
            t = it - 1
            o = jnp.where(it == 0, 1024, jnp.where(t < 2, 1 - cc, cc) * OWN + 256 * lax.rem(t + 2, 2))
            qs = jnp.where(ci == 0, o, 256 * b)
            q0 = jnp.where(ci == 0, o, 256 + 256 * b)
            part = (ci == 0) | (p == 0)
            kp = jnp.where(ci == 0, 0, jnp.where(p == 0, 1024, 512 * (p - 1)))
            full = jnp.where(part, lax.div(q0, 512), 1)
            small = jnp.where(part, 1 + lax.rem(lax.div(q0, 256), 2), 0)
            attend(_al(qs, 256), jnp.where(ci == 0, 0, b), kp, full, small, 256 - 256 * small, part, (ci == 0) | (p == 2))

            @pl.when((ci == 0) & (it == 0))
            def _():
                send_o(_al(1024 + 128 * (1 - cc), 128), 128, OWN, 8).start()

            @pl.when((ci == 0) & (it > 0) & (it < 3))
            def _():
                send_o(_al(qs, 256), 256, _al(256 * t, 256), 8 + it).start()

            @pl.when((ci == 1) & (p == 2) & (it < 2 - cc))
            def _():
                send_o(_al(qs, 256), 256, _al(256 * it + 256 * cc, 256), 9 + it).start()

        n_att = jnp.where(ci == 1, 3, jnp.where(p == 1, 5, 0))
        lax.fori_loop(0, n_att, att, None)

    lax.fori_loop(0, 3, phase, None)

    get_wo.wait()
    get_wo2.wait()

    def put(o, slot):
        return local(xs.at[pl.ds(slot, 128)], y_ref.at[pl.ds(slot, 128)], 6 + o)

    def slot_of(o):
        s0 = jnp.where(o == 0, OWN, 128 * (o - 1))
        return _al(jnp.where(ci == 0, s0, jnp.where(cc == 0, 256, 0) + 128 * o), 128)

    def out(o, _):
        @pl.when((ci == 0) & (o == 0))
        def _():
            send_o(0, 128, OWN, 8).wait_recv()

        @pl.when(((ci == 0) & (o == 1)) | ((ci == 1) & (o == 0)))
        def _():
            send_o(0, 256, 0, 9).wait_recv()

        @pl.when(((ci == 0) & (o == 1)) | ((ci == 1) & (o == 0) & (cc == 1)))
        def _():
            send_o(0, 256, 0, 10).wait_recv()

        slot = slot_of(o)
        s0 = jnp.where(o == 0, 1024 + 128 * cc, OWN * cc + 128 * (o - 1))
        qs = _al(jnp.where(ci == 0, s0, OWN * cc + slot - 256), 128)
        for n in range(8):
            at = slice(256 * n, 256 * n + 256)
            t = _dot(qo[pl.ds(qs, 128), :], wqo[:, at], 1, 0) + _dot(ox[pl.ds(slot, 128), :], wkv[:, at], 1, 0)
            xs[pl.ds(slot, 128), at] = (xs[pl.ds(slot, 128), at].astype(jnp.float32) + t).astype(jnp.bfloat16)

        @pl.when((ci == 0) & (o == 0))
        def _():
            send_yt(cc).start()

        @pl.when((ci == 1) | (o > 0))
        def _():
            put(o, slot).start()

    n_out = jnp.where(ci == 0, 5, jnp.where(cc == 0, 2, 4))
    lax.fori_loop(0, n_out, out, None)

    def done(o, _):
        put(o, slot_of(o)).wait()

    lax.fori_loop(jnp.where(ci == 0, 1, 0), n_out, done, None)
    send_a.wait_send()

    @pl.when(ci == 0)
    def _():
        send_far(0).wait_send()
        send_far(1).wait_send()
        send_at.wait_send()
        send_o(0, 128, OWN, 8).wait_send()
        send_o(0, 256, 0, 9).wait_send()
        send_o(0, 256, 0, 10).wait_send()
        send_yt(cc).wait_send()

    @pl.when(ci == 1)
    def _():
        relay(0).wait_send()
        relay(1).wait_send()
        send_o(0, 256, 0, 9).wait_send()

    @pl.when(me == 2)
    def _():
        send_o(0, 256, 0, 10).wait_send()
        send_xt(0).wait_send()
        send_xt(1).wait_send()
        send_yt(0).wait_recv()
        send_yt(1).wait_recv()


def _tables():
    freq = THETA ** (-np.arange(64) / 64.0)
    sign = np.concatenate([-np.ones(64), np.ones(64)])

    def both(place):
        angle = np.tile(place[:, None] * freq, (1, 2))
        return np.concatenate([np.cos(angle), np.sin(angle) * sign]).astype(np.float32)

    return both(128.0 * np.arange(16)), both(np.arange(128.0))


def solution(mesh):
    hi, lo = _tables()
    any_, vmem = pl.BlockSpec(memory_space=pl.ANY), pl.BlockSpec(memory_space=pltpu.VMEM)
    bf, f32 = jnp.bfloat16, jnp.float32

    def step(x, gain, wq, wk, wv, wo):
        return pl.pallas_call(
            _kernel,
            out_shape=jax.ShapeDtypeStruct(x.shape, bf),
            in_specs=[any_, vmem, vmem, vmem, any_, any_, any_, any_],
            out_specs=any_,
            scratch_shapes=[
                pltpu.VMEM((OWN + 128, D), bf),
                pltpu.VMEM((2048, D), bf),
                pltpu.VMEM((D, D), bf),
                pltpu.VMEM((D, D), bf),
                pltpu.VMEM((KVH, 2048, HEAD), bf),
                pltpu.VMEM((KVH, HEAD + 16, 2048), bf),
                pltpu.VMEM((1024 + TM, D), bf),
                pltpu.VMEM((OWN + 128, D), bf),
                pltpu.VMEM((3, KVH, 1, COLS), f32),
                pltpu.VMEM((3, KVH, HEAD + 8, COLS), f32),
                pltpu.SemaphoreType.DMA((11,)),
                pltpu.SemaphoreType.DMA((15,)),
                pltpu.SemaphoreType.DMA((15,)),
            ],
            compiler_params=pltpu.CompilerParams(collective_id=0, has_side_effects=True, vmem_limit_bytes=67043328),
        )(x, gain.reshape(1, D), jnp.asarray(hi), jnp.asarray(lo), wq, wk, wv, wo)

    tokens, whole = P(("dp", "sp"), None), P(None, None)
    return jax.shard_map(step, mesh=mesh, in_specs=(tokens, P(None), whole, whole, whole, whole), out_specs=tokens, check_vma=False)
```

```python
import functools

import jax
import jax.numpy as jnp
import numpy as np
from jax import lax
from jax.experimental import pallas as pl
from jax.experimental.pallas import tpu as pltpu
from jax.sharding import PartitionSpec as P

HEAD = 128
THETA = 10000
NEG = -1e30
HIDDEN = 2 * NEG
LOG2E = 1.4426950408889634
E = HEAD**-0.5 * LOG2E
D = 2048
KVH = 8
GRP = 4
BQ = 256
BK = 512
COLS = 2 * BQ
OWN = 512
TM = 256
MESH = pl.DeviceIdType.MESH


def _dot(a, b, ca, cb):
    return lax.dot_general(a, b, (((ca,), (cb,)), ((), ())), preferred_element_type=jnp.float32)


def _al(v, n):
    return pl.multiple_of(v, n)


def _kernel(x_ref, gain_ref, hi_ref, lo_ref, wq_ref, wk_ref, wv_ref, wo_ref, xs,
            ab, wkv, wqo, kb, vt, qo, ox, top, mix, sa, sb, ma, mb, loc, snd, rcv):
    me = lax.axis_index("sp")
    ci, cc = lax.div(me, 2), lax.rem(me, 2)
    par = 2 * ci + 1 - cc
    far = 2 * (1 - ci) + cc

    def local(src, dst, i):
        return pltpu.make_async_copy(src, dst, loc.at[i])

    def remote(src, dst, i, to, s=None):
        return pltpu.make_async_remote_copy(src_ref=src, dst_ref=dst, send_sem=snd.at[i if s is None else s], recv_sem=rcv.at[i],
                                            device_id={"sp": to}, device_id_type=MESH)

    get_x = local(x_ref, xs.at[pl.ds(0, OWN)], 0)
    get_wk = local(wk_ref.at[:, pl.ds(_al(cc * 1024, 1024), 1024)], wkv.at[:, pl.ds(0, 1024)], 1)
    get_wv = local(wv_ref.at[:, pl.ds(_al(cc * 1024, 1024), 1024)], wkv.at[:, pl.ds(1024, 1024)], 2)
    get_wq = local(wq_ref.at[:, pl.ds(_al(cc * D, D), D)], wqo, 3)
    get_wo = local(wo_ref.at[pl.ds(_al(cc * D, D), D)], wqo, 4)
    get_wo2 = local(wo_ref.at[pl.ds(_al((1 - cc) * D, D), D)], wkv, 5)
    get_x.start()
    get_wk.start()
    get_wv.start()

    barrier = pltpu.get_barrier_semaphore()
    for k in range(1, 4):
        pl.semaphore_signal(barrier, inc=1, device_id={"sp": lax.rem(me + k, 4)}, device_id_type=MESH)
    pl.semaphore_wait(barrier, 3)

    mine = _al(me * OWN, OWN)
    theirs = _al(par * OWN, OWN)
    send_a = remote(ab.at[pl.ds(mine, OWN)], ab.at[pl.ds(mine, OWN)], 0, par)

    def send_far(h):
        at = pl.ds(_al(cc * OWN + h * 256, 256), 256)
        return remote(ab.at[at], ab.at[at], 1 + h, far)

    def relay(h):
        at = pl.ds(_al(cc * OWN + h * 256, 256), 256)
        return remote(ab.at[at], ab.at[at], 3 + h, par)

    def send_xt(k):
        return remote(x_ref.at[pl.ds(128 * k, 128)], xs.at[pl.ds(OWN, 128)], 5, k, 5 + k)

    at_t = pl.ds(_al(1024 + cc * 128, 128), 128)
    send_at = remote(ab.at[at_t], ab.at[at_t], 7, par)

    def send_o(src, rows, dst, i):
        return remote(qo.at[pl.ds(src, rows)], ox.at[pl.ds(dst, rows)], i, par)

    send_xm = remote(x_ref.at[pl.ds(0, 128)], xs.at[pl.ds(OWN, 128)], 5, 2)

    def send_y(c):
        return remote(xs.at[pl.ds(OWN, 128)], xs.at[pl.ds(_al(128 * c, 128), 128)], 13 + c, jnp.where(ci == 0, 2, 3))

    def norm(src, dst, rows):
        gain = gain_ref[...].astype(jnp.float32).reshape(1, D)

        def some(j, _):
            for k in range(4):
                wide = xs[pl.ds(_al(src + 64 * j + 16 * k, 16), 16), :].astype(jnp.float32)
                scale = lax.rsqrt(jnp.mean(wide * wide, -1, keepdims=True) + 1e-6)
                ab[pl.ds(_al(dst + 64 * j + 16 * k, 16), 16), :] = (wide * scale * gain).astype(jnp.bfloat16)
        lax.fori_loop(0, rows // 64, some, None)

    get_x.wait()
    norm(0, mine, OWN)
    send_a.start()

    @pl.when(ci == 0)
    def _():
        send_far(0).start()
        send_far(1).start()

    @pl.when(me == 2)
    def _():
        send_xt(0).start()
        send_xt(1).start()

    @pl.when(me == 3)
    def _():
        send_xm.start()

    for h in range(KVH):
        vt[h, HEAD:, :] = jnp.ones((16, D), jnp.bfloat16)
        for slot in range(3):
            mix[slot, h] = jnp.zeros((HEAD + 8, COLS), jnp.float32)

    def angles(r):
        cl, sl = lo_ref[:128, :], lo_ref[128:, :]
        cs, ss = [], []
        for k in range(2):
            n = lax.div(r, 128) + k
            ch, sh = hi_ref[pl.ds(n, 1), :], hi_ref[pl.ds(16 + n, 1), :]
            cs.append(ch * cl - sh * sl)
            ss.append(sh * cl + ch * sl)
        return jnp.concatenate(cs, 0), jnp.concatenate(ss, 0)

    def turned(t, cos, sin):
        t = t.astype(jnp.bfloat16).astype(jnp.float32)
        return (t * cos + pltpu.roll(t, 64, 1) * sin).astype(jnp.bfloat16)

    def kv_step(r, pos):
        cos, sin = angles(r)
        for n in range(4):
            t = _dot(ab[pl.ds(r, 256), :], wkv[:, 256 * n : 256 * n + 256], 1, 0)
            for k in range(2):
                kb[2 * n + k, pl.ds(pos, 256), :] = turned(t[:, 128 * k : 128 * k + 128], cos, sin)
        for n in range(4):
            t = _dot(ab[pl.ds(r, 256), :], wkv[:, 1024 + 256 * n : 1024 + 256 * n + 256], 1, 0).astype(jnp.bfloat16)
            for k in range(2):
                vt[2 * n + k, :HEAD, pl.ds(pos, 256)] = t[:, 128 * k : 128 * k + 128].T

    def q_step(r, pos):
        cos, sin = angles(r)
        for n in range(8):
            t = _dot(ab[pl.ds(r, 256), :], wqo[:, 256 * n : 256 * n + 256], 1, 0)
            for k in range(2):
                qo[pl.ds(pos, 256), 256 * n + 128 * k : 256 * n + 128 * k + 128] = turned(t[:, 128 * k : 128 * k + 128], cos, sin)

    def scores(buf, most, g, qs, at, level):
        if level is not None:
            gap = lax.rem(lax.broadcasted_iota(jnp.int32, (BK, COLS), 1), BQ) - lax.broadcasted_iota(jnp.int32, (BK, COLS), 0)
            ok = gap >= level
        for i in range(GRP):
            h = g * GRP + i
            q = jnp.concatenate([qo[pl.ds(qs, BQ), 256 * h + HEAD * n : 256 * h + HEAD * n + HEAD] for n in range(2)], 0)
            s = _dot(kb[h, pl.ds(at, BK), :], q, 1, 1)
            if level is not None:
                s = jnp.where(ok, s, HIDDEN)
            buf[i] = s
            most[i] = s.max(axis=0, keepdims=True)

    def weigh(buf, most, g, slot, at):
        for i in range(GRP):
            h = g * GRP + i
            old = top[slot, h]
            new = jnp.maximum(old, most[i])
            top[slot, h] = new
            p = jnp.exp2((buf[i] - new) * E).astype(jnp.bfloat16)
            add = _dot(vt[h, :, pl.ds(at, BK)], p, 1, 0)
            mix[slot, h] = mix[slot, h] * jnp.exp2((old - new) * E) + add[: HEAD + 8]

    def attend(qs, slot, kp, full, part, level, begin, end, qs_next, kp_next, level_next):
        @pl.when(begin)
        def _():
            for h in range(KVH):
                top[slot, h] = jnp.full((1, COLS), NEG, jnp.float32)

        def block(j, masked):
            at = _al(kp + BK * j, 256)
            last = j == full + part - 1
            level_j = jnp.where(j == full, level, -BK) if masked else None
            level_n = jnp.where(last, level_next, jnp.where(j == full - 1, level, -BK)) if masked else None
            scores(sb, mb, 1, qs, at, level_j)
            weigh(sa, ma, 0, slot, at)
            scores(sa, ma, 0, _al(jnp.where(last, qs_next, qs), 256), _al(jnp.where(last, kp_next, at + BK), 256), level_n)
            weigh(sb, mb, 1, slot, at)

        clear = jnp.maximum(full - part, 0)
        lax.fori_loop(0, clear, lambda j, _: block(j, False), None)
        lax.fori_loop(clear, full + part, lambda j, _: block(j, True), None)

        @pl.when(end)
        def _():
            for h in range(KVH):
                total = mix[slot, h, HEAD : HEAD + 1, :]
                out = (mix[slot, h, :HEAD, :] * (1 / total)).T.astype(jnp.bfloat16)
                for n in range(2):
                    qo[pl.ds(qs, BQ), 256 * h + HEAD * n : 256 * h + HEAD * n + HEAD] = out[BQ * n : BQ * n + BQ]

    def phase(p, _):
        late = (ci == 1) & (p >= 1)

        @pl.when(late)
        def _():
            send_far(p - 1).wait_recv()
            relay(p - 1).start()

        def kv(j, _):
            @pl.when((p == 0) & (j == 0))
            def _():
                get_wk.wait()
                get_wv.wait()
                get_wq.start()

            @pl.when((p == 0) & (j == 2))
            def _():
                send_a.wait_recv()

            @pl.when((p == 1) & (ci == 0))
            def _():
                send_at.wait_recv()

            @pl.when(late & (j == 1))
            def _():
                relay(p - 1).wait_recv()

            first = jnp.where(p == 0, 1, 0)
            jj, jh = lax.rem(j, 2), lax.div(j, 2)
            r0 = jnp.where(jh == 0, me, par) * OWN + 256 * jj
            r1 = jnp.where(ci == 0, 1024, jnp.where(j == 0, cc, 1 - cc) * OWN + 256 * (p - 1))
            r = jnp.where(first == 1, r0, r1)
            pos = jnp.where((first == 1) | (ci == 0), r, 512 * (p - 1) + 256 * j)
            kv_step(_al(r, 256), _al(pos, 256))

        n_kv = jnp.where(p == 0, 4, jnp.where(ci == 1, 2, jnp.where(p == 1, 1, 0)))
        lax.fori_loop(0, n_kv, kv, None)

        @pl.when(p == 1 + ci)
        def _():
            get_wo2.start()

        def q(j, _):
            @pl.when((p == 0) & (j == 0))
            def _():
                get_wq.wait()

            @pl.when((p == 0) & (ci == 0) & (j == 2))
            def _():
                send_xt(0).wait_recv()
                norm(OWN, 1024 + cc * 128, 128)
                send_at.start()

            pos = jnp.where(p == 0, 256 * j, 1024)
            q_step(_al(pos + 1280 * ci, 256), _al(pos, 256))

        n_q = jnp.where(p == 0, 4 - ci, jnp.where((p == 1) & (ci == 0), 1, 0))
        lax.fori_loop(0, n_q, q, None)

        @pl.when(p == 1 - ci)
        def _():
            get_wo.start()

        def item(it):
            b = lax.rem(it + 1 - cc, 3)
            t = it - 1
            o = jnp.where(it == 0, 1024, jnp.where(t < 2, 1 - cc, cc) * OWN + 256 * lax.rem(t + 2, 2))
            qs = jnp.where(ci == 0, o, 256 * b)
            q0 = jnp.where(ci == 0, o, 256 + 256 * b)
            return t, b, _al(qs, 256), q0

        own_keys = (ci == 0) | (p == 0)
        kp = _al(jnp.where(ci == 0, 0, jnp.where(p == 0, 1024, 512 * (p - 1))), 512)
        n_att = jnp.where(ci == 1, 3, jnp.where(p == 1, 5, 0))

        def first_level(q0):
            return jnp.where(own_keys & (q0 < 512), -q0, -BK)

        @pl.when(n_att > 0)
        def _():
            _, _, qs, q0 = item(0)
            scores(sa, ma, 0, qs, kp, first_level(q0))

        def att(it, _):
            t, b, qs, q0 = item(it)
            full = jnp.where(own_keys, lax.div(q0, 512), 1)
            part = jnp.where(own_keys, 1, 0)
            _, _, qs_next, q0_next = item(jnp.minimum(it + 1, n_att - 1))
            attend(qs, jnp.where(ci == 0, 0, b), kp, full, part, -lax.rem(q0, 512), own_keys, (ci == 0) | (p == 2),
                   qs_next, kp, first_level(q0_next))

            @pl.when((ci == 0) & (it == 0))
            def _():
                send_o(_al(1024 + 128 * (1 - cc), 128), 128, OWN, 8).start()

            @pl.when((ci == 0) & (it > 0) & (it < 3))
            def _():
                send_o(_al(qs, 256), 256, _al(256 * t, 256), 8 + it).start()

            @pl.when((ci == 1) & (p == 2) & (((cc == 0) & (it == 1)) | ((cc == 1) & (it == 0))))
            def _():
                send_o(qs, 256, 256, 10 - cc).start()

            @pl.when((ci == 1) & (p == 2) & (((cc == 0) & (it == 0)) | ((cc == 1) & (it == 1))))
            def _():
                send_o(_al(qs + 128 * (1 - cc), 128), 128, _al(128 + 384 * cc, 128), 9 - cc).start()

        lax.fori_loop(0, n_att, att, None)

    lax.fori_loop(0, 3, phase, None)

    get_wo.wait()
    get_wo2.wait()

    def out(o, _):
        moved = (o == 0) & (me < 3)

        @pl.when((o == 0) & (me != 3))
        def _():
            send_o(0, 128, OWN, 8).wait_recv()

        @pl.when(((ci == 0) & (o == 1)) | ((me == 2) & (o == 1)))
        def _():
            send_o(0, 256, 0, 9).wait_recv()

        @pl.when((me == 3) & (o == 0))
        def _():
            send_o(0, 128, 128, 9).wait_recv()

        @pl.when(((ci == 0) & (o == 1)) | ((me == 3) & (o == 1)))
        def _():
            send_o(0, 256, 0, 10).wait_recv()

        @pl.when((me == 2) & (o == 0))
        def _():
            send_xm.wait_recv()

        kept = jnp.where(ci == 0, 128 * (o - 1), 128 + 128 * o)
        slot = _al(jnp.where(moved, OWN, kept), 128)
        first = jnp.where(ci == 0, OWN * cc, OWN * cc - 256)
        qs = _al(jnp.where(moved, jnp.where(ci == 0, 1024 + 128 * cc, 256), first + kept), 128)
        for n in range(8):
            at = slice(256 * n, 256 * n + 256)
            t = _dot(qo[pl.ds(qs, 128), :], wqo[:, at], 1, 0) + _dot(ox[pl.ds(slot, 128), :], wkv[:, at], 1, 0)
            xs[pl.ds(slot, 128), at] = (xs[pl.ds(slot, 128), at].astype(jnp.float32) + t).astype(jnp.bfloat16)

        @pl.when(moved)
        def _():
            send_y(cc).start()

    lax.fori_loop(0, jnp.where(ci == 0, 5, 3), out, None)

    send_a.wait_send()

    @pl.when(ci == 0)
    def _():
        send_far(0).wait_send()
        send_far(1).wait_send()
        send_at.wait_send()
        send_o(0, 128, OWN, 8).wait_send()
        send_o(0, 256, 0, 9).wait_send()
        send_o(0, 256, 0, 10).wait_send()
        send_y(cc).wait_send()

    @pl.when(ci == 1)
    def _():
        relay(0).wait_send()
        relay(1).wait_send()

    @pl.when(me == 2)
    def _():
        send_o(0, 128, 128, 9).wait_send()
        send_o(0, 256, 256, 10).wait_send()
        send_xt(0).wait_send()
        send_xt(1).wait_send()
        send_y(0).wait_send()
        send_y(0).wait_recv()
        send_y(1).wait_recv()

    @pl.when(me == 3)
    def _():
        send_o(0, 256, 256, 9).wait_send()
        send_o(0, 128, OWN, 8).wait_send()
        send_xm.wait_send()
        send_y(0).wait_recv()


def _tables():
    freq = THETA ** (-np.arange(64) / 64.0)
    sign = np.concatenate([-np.ones(64), np.ones(64)])

    def both(place):
        angle = np.tile(place[:, None] * freq, (1, 2))
        return np.concatenate([np.cos(angle), np.sin(angle) * sign]).astype(np.float32)

    return both(128.0 * np.arange(16)), both(np.arange(128.0))


def solution(mesh):
    hi, lo = _tables()
    any_, vmem = pl.BlockSpec(memory_space=pl.ANY), pl.BlockSpec(memory_space=pltpu.VMEM)
    bf, f32 = jnp.bfloat16, jnp.float32

    def step(x, gain, wq, wk, wv, wo):
        out = pl.pallas_call(
            _kernel,
            out_shape=pltpu.VMEM((OWN + 128, D), bf),
            in_specs=[any_, vmem, vmem, vmem, any_, any_, any_, any_],
            out_specs=vmem,
            scratch_shapes=[
                pltpu.VMEM((2048, D), bf),
                pltpu.VMEM((D, D), bf),
                pltpu.VMEM((D, D), bf),
                pltpu.VMEM((KVH, 2048, HEAD), bf),
                pltpu.VMEM((KVH, HEAD + 16, 2048), bf),
                pltpu.VMEM((1024 + TM, D), bf),
                pltpu.VMEM((OWN + 128, D), bf),
                pltpu.VMEM((3, KVH, 1, COLS), f32),
                pltpu.VMEM((3, KVH, HEAD + 8, COLS), f32),
                pltpu.VMEM((GRP, BK, COLS), f32),
                pltpu.VMEM((GRP, BK, COLS), f32),
                pltpu.VMEM((GRP, 1, COLS), f32),
                pltpu.VMEM((GRP, 1, COLS), f32),
                pltpu.SemaphoreType.DMA((11,)),
                pltpu.SemaphoreType.DMA((15,)),
                pltpu.SemaphoreType.DMA((15,)),
            ],
            compiler_params=pltpu.CompilerParams(collective_id=0, has_side_effects=True, vmem_limit_bytes=60 * 2**20),
        )(x, gain, jnp.asarray(hi), jnp.asarray(lo), wq, wk, wv, wo)
        return out[:OWN]

    tokens, whole = P(("dp", "sp"), None), P(None, None)
    return jax.shard_map(step, mesh=mesh, in_specs=(tokens, P(None), whole, whole, whole, whole), out_specs=tokens, check_vma=False)
```

```python
import functools

import jax
import jax.numpy as jnp
import numpy as np
from jax import lax
from jax.experimental import pallas as pl
from jax.experimental.pallas import tpu as pltpu
from jax.sharding import PartitionSpec as P

HEAD = 128
THETA = 10000
NEG = -1e30
HIDDEN = 2 * NEG
SEEN = 3e38
ALL, SECOND, FIRST = 0, 256, 512
LOG2E = 1.4426950408889634
E = HEAD**-0.5 * LOG2E
D = 2048
KVH = 8
BQ = 256
BK = 512
COLS = 2 * BQ
OWN = 512
TM = 256
MESH = pl.DeviceIdType.MESH


def _dot(a, b, ca, cb):
    return lax.dot_general(a, b, (((ca,), (cb,)), ((), ())), preferred_element_type=jnp.float32)


def _al(v, n):
    return pl.multiple_of(v, n)


def _kernel(x_ref, gain_ref, hi_ref, lo_ref, wq_ref, wk_ref, wv_ref, wo_ref, xs,
            ab, wkv, wqo, kb, vt, qo, ox, top, mix, sa, sb, ma, mb, vis, loc, snd, rcv):
    me = lax.axis_index("sp")
    ci, cc = lax.div(me, 2), lax.rem(me, 2)
    par = 2 * ci + 1 - cc
    far = 2 * (1 - ci) + cc

    def local(src, dst, i):
        return pltpu.make_async_copy(src, dst, loc.at[i])

    def remote(src, dst, i, to, s=None):
        return pltpu.make_async_remote_copy(src_ref=src, dst_ref=dst, send_sem=snd.at[i if s is None else s], recv_sem=rcv.at[i],
                                            device_id={"sp": to}, device_id_type=MESH)

    get_x = local(x_ref, xs.at[pl.ds(0, OWN)], 0)
    get_wk = local(wk_ref.at[:, pl.ds(_al(cc * 1024, 1024), 1024)], wkv.at[:, pl.ds(0, 1024)], 1)
    get_wv = local(wv_ref.at[:, pl.ds(_al(cc * 1024, 1024), 1024)], wkv.at[:, pl.ds(1024, 1024)], 2)
    get_wq = local(wq_ref.at[:, pl.ds(_al(cc * D, D), D)], wqo, 3)
    get_wo = local(wo_ref.at[pl.ds(_al(cc * D, D), D)], wqo, 4)
    get_wo2 = local(wo_ref.at[pl.ds(_al((1 - cc) * D, D), D)], wkv, 5)
    get_x.start()
    get_wk.start()
    get_wv.start()

    barrier = pltpu.get_barrier_semaphore()
    for k in range(1, 4):
        pl.semaphore_signal(barrier, inc=1, device_id={"sp": lax.rem(me + k, 4)}, device_id_type=MESH)
    pl.semaphore_wait(barrier, 3)

    mine = _al(me * OWN, OWN)
    theirs = _al(par * OWN, OWN)
    send_a = remote(ab.at[pl.ds(mine, OWN)], ab.at[pl.ds(mine, OWN)], 0, par)

    def send_far(c):
        return remote(ab.at[pl.ds(_al(mine + 128 * c, 128), 128)], ab.at[pl.ds(_al(256 * c + 128 * cc, 128), 128)], 16 + c, far)

    def relay(c):
        at = pl.ds(_al(256 * c + 128 * cc, 128), 128)
        return remote(ab.at[at], ab.at[at], 20 + c, par)

    def send_xt(k):
        return remote(x_ref.at[pl.ds(128 * k, 128)], xs.at[pl.ds(OWN, 128)], 5, k, 5 + k)

    at_t = pl.ds(_al(1024 + cc * 128, 128), 128)
    send_at = remote(ab.at[at_t], ab.at[at_t], 7, par)

    def send_o(src, rows, dst, i):
        return remote(qo.at[pl.ds(src, rows)], ox.at[pl.ds(dst, rows)], i, par)

    send_xm = remote(x_ref.at[pl.ds(0, 128)], xs.at[pl.ds(OWN, 128)], 5, 2)

    def send_y(c):
        return remote(xs.at[pl.ds(OWN, 128)], xs.at[pl.ds(_al(128 * c, 128), 128)], 13 + c, jnp.where(ci == 0, 2, 3))

    def norm(ref, src, dst, rows):
        gain = gain_ref[...].astype(jnp.float32).reshape(1, D)

        def some(j, _):
            for k in range(4):
                wide = ref[pl.ds(_al(src + 64 * j + 16 * k, 16), 16), :].astype(jnp.float32)
                scale = lax.rsqrt(jnp.mean(wide * wide, -1, keepdims=True) + 1e-6)
                ab[pl.ds(_al(dst + 64 * j + 16 * k, 16), 16), :] = (wide * scale * gain).astype(jnp.bfloat16)
        lax.fori_loop(0, rows // 64, some, None)

    get_x.wait()
    for c in range(4):
        norm(xs, 128 * c, mine + 128 * c, 128)

        @pl.when(ci == 0)
        def _():
            send_far(c).start()

    send_a.start()

    @pl.when(me == 2)
    def _():
        send_xt(0).start()
        send_xt(1).start()

    @pl.when(me == 3)
    def _():
        send_xm.start()

    for h in range(KVH):
        vt[h, HEAD:, :] = jnp.ones((16, D), jnp.bfloat16)
        for slot in range(3):
            mix[slot, h] = jnp.zeros((HEAD + 8, COLS), jnp.float32)

    for j in range(4):
        key = lax.broadcasted_iota(jnp.int32, (256, BQ), 0) + (256 * j - BK)
        vis[256 * j : 256 * j + 256, :] = jnp.where(key <= lax.broadcasted_iota(jnp.int32, (256, BQ), 1), SEEN, HIDDEN)

    def angles(*places):
        cl, sl = lo_ref[:128, :], lo_ref[128:, :]
        cs, ss = [], []
        for n in places:
            ch, sh = hi_ref[pl.ds(n, 1), :], hi_ref[pl.ds(16 + n, 1), :]
            cs.append(ch * cl - sh * sl)
            ss.append(sh * cl + ch * sl)
        return jnp.concatenate(cs, 0), jnp.concatenate(ss, 0)

    def turned(t, cos, sin):
        t = t.astype(jnp.bfloat16).astype(jnp.float32)
        return (t * cos + pltpu.roll(t, 64, 1) * sin).astype(jnp.bfloat16)

    def kv_step(*runs):
        turns = [angles(*n) for _, *n in runs]
        for n in range(4):
            for (r, *_), (cos, sin) in zip(runs, turns):
                t = _dot(ab[pl.ds(r, 256), :], wkv[:, 1024 + 256 * n : 1024 + 256 * n + 256], 1, 0).astype(jnp.bfloat16)
                for k in range(2):
                    vt[2 * n + k, :HEAD, pl.ds(r, 256)] = t[:, 128 * k : 128 * k + 128].T
        for n in range(4):
            for (r, *_), (cos, sin) in zip(runs, turns):
                t = _dot(ab[pl.ds(r, 256), :], wkv[:, 256 * n : 256 * n + 256], 1, 0)
                for k in range(2):
                    kb[2 * n + k, pl.ds(r, 256), :] = turned(t[:, 128 * k : 128 * k + 128], cos, sin)

    def q_step(r, pos):
        n = lax.div(r, 128)
        cos, sin = angles(n, n + 1)
        for n in range(8):
            t = _dot(ab[pl.ds(r, 256), :], wqo[:, 256 * n : 256 * n + 256], 1, 0)
            for k in range(2):
                qo[pl.ds(pos, 256), 256 * n + 128 * k : 256 * n + 128 * k + 128] = turned(t[:, 128 * k : 128 * k + 128], cos, sin)

    bufs = (sa, ma), (sb, mb)

    def scores(buf, most, h, qs, at, keys, view=None, k=0):
        q = jnp.concatenate([qo[pl.ds(qs, BQ), 256 * h + HEAD * n : 256 * h + HEAD * n + HEAD] for n in range(2)], 0)
        s = _dot(kb[h, pl.ds(at, keys), :], q, 1, 1)
        if view is not None:
            bound = vis[pl.ds(_al(view, 256), keys), :]
            s = jnp.minimum(s, jnp.concatenate([bound, bound], 1))
        buf[keys * k : keys * k + keys] = s
        most[k] = s.max(axis=0, keepdims=True)

    def weigh(buf, most, h, slot, at, keys, k=0):
        old = top[slot, h]
        new = jnp.maximum(old, most[k])
        top[slot, h] = new
        p = jnp.exp2((buf[keys * k : keys * k + keys] - new) * E).astype(jnp.bfloat16)
        add = _dot(vt[h, :, pl.ds(at, keys)], p, 1, 0)
        mix[slot, h] = mix[slot, h] * jnp.exp2((old - new) * E) + add[: HEAD + 8]

    def attend(qs, slot, kp, full, part, few, view, begin, end, qs_next, kp_next, view_next):
        @pl.when(begin)
        def _():
            for h in range(KVH):
                top[slot, h] = jnp.full((1, COLS), NEG, jnp.float32)

        def block(j, keys, view_j):
            at = _al(kp + BK * j, 256)
            last = j == full + part - 1
            view_n = jnp.where(last, view_next, jnp.where((j == full - 1) & (part == 1), view, ALL))
            for h in range(KVH):
                if h < KVH - 1:
                    scores(*bufs[(h + 1) % 2], h + 1, qs, at, keys, view_j)
                else:
                    scores(*bufs[0], 0, _al(jnp.where(last, qs_next, qs), 256), _al(jnp.where(last, kp_next, at + BK), 256), BK, view_n)
                weigh(*bufs[h % 2], h, slot, at, keys)

        lax.fori_loop(0, full, lambda j, _: block(j, BK, None), None)

        @pl.when(few)
        def _():
            for g in range(KVH // 2):
                more = g < KVH // 2 - 1
                for k in range(2):
                    scores(*bufs[(g + 1) % 2], 2 * g + 2 + k if more else k, qs if more else qs_next, kp if more else kp_next, 256, k=k)
                for k in range(2):
                    weigh(*bufs[g % 2], 2 * g + k, slot, kp, 256, k)

        @pl.when((part == 1) & (view == FIRST))
        def _():
            block(full, 256, FIRST)

        @pl.when((part == 1) & (view == SECOND))
        def _():
            block(full, BK, SECOND)

        @pl.when(end)
        def _():
            for h in range(KVH):
                total = mix[slot, h, HEAD : HEAD + 1, :]
                out = (mix[slot, h, :HEAD, :] * (1 / total)).T.astype(jnp.bfloat16)
                for n in range(2):
                    qo[pl.ds(qs, BQ), 256 * h + HEAD * n : 256 * h + HEAD * n + HEAD] = out[BQ * n : BQ * n + BQ]

    def pass_on(c):
        send_far(c).wait_recv()
        relay(c).start()

    def phase(p, _):
        def kv(j, _):
            @pl.when((p == 0) & (j == 0))
            def _():
                get_wk.wait()
                get_wv.wait()
                get_wq.start()

            @pl.when((p == 0) & (j == 1))
            def _():
                send_a.wait_recv()

            @pl.when(p == 1)
            def _():
                relay(0).wait_recv()
                relay(1).wait_recv()

            ra = _al(jnp.where(p == 0, jnp.where(j == 0, me, par) * OWN, 0), OWN)
            na = lax.div(ra, 128)
            kv_step((ra, na, jnp.where(p == 0, na + 1, 4)), (_al(ra + 256, 256), jnp.where(p == 0, na + 2, 1), jnp.where(p == 0, na + 3, 5)))

        lax.fori_loop(0, jnp.where(p == 0, 2, jnp.where((ci == 1) & (p == 1), 1, 0)), kv, None)

        @pl.when(((ci == 0) & (p == 1)) | ((ci == 1) & (p > 1)))
        def _():
            @pl.when(ci == 0)
            def _():
                send_at.wait_recv()

            @pl.when(ci == 1)
            def _():
                relay(p).wait_recv()

            kv_step((_al(jnp.where(ci == 0, 1024, 256 * p), 256), jnp.where(ci == 0, 8, p), jnp.where(ci == 0, 9, 4 + p)))

        @pl.when(p == 1 + 2 * ci)
        def _():
            get_wo2.start()

        def q(j, _):
            @pl.when((p == 0) & (j == 0))
            def _():
                get_wq.wait()

            @pl.when((p == 0) & (ci == 0) & (j == 2))
            def _():
                send_xt(0).wait_recv()
                norm(xs, OWN, 1024 + cc * 128, 128)
                send_at.start()

            pos = jnp.where(p == 0, 256 * j, 1024)
            q_step(_al(pos + 1280 * ci, 256), _al(pos, 256))

        n_q = jnp.where(p == 0, 4 - ci, jnp.where((p == 1) & (ci == 0), 1, 0))
        lax.fori_loop(0, n_q, q, None)

        @pl.when(p == 1 - ci)
        def _():
            get_wo.start()

        def item(it):
            b = lax.rem(it + 1 - cc, 3)
            t = it - 1
            o = jnp.where(it == 0, 1024, jnp.where(t < 2, 1 - cc, cc) * OWN + 256 * lax.rem(t + 2, 2))
            qs = jnp.where(ci == 0, o, 256 * b)
            q0 = jnp.where(ci == 0, o, 256 + 256 * b)
            return t, b, _al(qs, 256), q0

        own_keys = (ci == 0) | (p == 0)
        kp = _al(jnp.where(ci == 0, 0, jnp.where(p == 0, 1024, jnp.where(p == 1, 0, 256 * p))), 256)
        n_att = jnp.where(ci == 1, 3, jnp.where(p == 1, 5, 0))

        def last_view(q0):
            return jnp.where(own_keys, jnp.where(lax.rem(q0, 512) == 0, FIRST, SECOND), ALL)

        def blocks(q0):
            return jnp.where(own_keys, lax.div(q0, 512), jnp.where(few, 0, 1))

        def first_view(q0):
            return jnp.where(blocks(q0) == 0, last_view(q0), ALL)

        few = p > 1

        @pl.when((n_att > 0) & few)
        def _():
            for k in range(2):
                scores(sa, ma, k, item(0)[2], kp, 256, k=k)

        @pl.when((n_att > 0) & jnp.logical_not(few))
        def _():
            _, _, qs, q0 = item(0)
            scores(sa, ma, 0, qs, kp, BK, first_view(q0))

        def att(it, _):
            t, b, qs, q0 = item(it)
            _, _, qs_next, q0_next = item(jnp.minimum(it + 1, n_att - 1))

            @pl.when((ci == 1) & (p == 0) & (it > 0))
            def _():
                pass_on(it - 1)

            @pl.when(((p == 1) | (p == 2)) & (ci == 1) & (it == 2))
            def _():
                pass_on(p + 1)

            attend(qs, jnp.where(ci == 0, 0, b), kp, blocks(q0), jnp.where(own_keys, 1, 0), few, last_view(q0), own_keys, (ci == 0) | (p == 3),
                   qs_next, kp, first_view(q0_next))

            @pl.when((ci == 0) & (it == 0))
            def _():
                send_o(_al(1024 + 128 * (1 - cc), 128), 128, OWN, 8).start()

            @pl.when((ci == 0) & (it > 0) & (it < 3))
            def _():
                send_o(_al(qs, 256), 256, _al(256 * t, 256), 8 + it).start()

            @pl.when((ci == 1) & (p == 3) & (((cc == 0) & (it == 1)) | ((cc == 1) & (it == 0))))
            def _():
                send_o(qs, 256, 256, 10 - cc).start()

            @pl.when((ci == 1) & (p == 3) & (((cc == 0) & (it == 0)) | ((cc == 1) & (it == 1))))
            def _():
                send_o(_al(qs + 128 * (1 - cc), 128), 128, _al(128 + 384 * cc, 128), 9 - cc).start()

        lax.fori_loop(0, n_att, att, None)

    lax.fori_loop(0, 4, phase, None)

    get_wo.wait()
    get_wo2.wait()

    def out(o, _):
        moved = (o == 0) & (me < 3)

        @pl.when((o == 0) & (me != 3))
        def _():
            send_o(0, 128, OWN, 8).wait_recv()

        @pl.when(((ci == 0) & (o == 1)) | ((me == 2) & (o == 1)))
        def _():
            send_o(0, 256, 0, 9).wait_recv()

        @pl.when((me == 3) & (o == 0))
        def _():
            send_o(0, 128, 128, 9).wait_recv()

        @pl.when(((ci == 0) & (o == 1)) | ((me == 3) & (o == 1)))
        def _():
            send_o(0, 256, 0, 10).wait_recv()

        @pl.when((me == 2) & (o == 0))
        def _():
            send_xm.wait_recv()

        kept = jnp.where(ci == 0, 128 * (o - 1), 128 + 128 * o)
        slot = _al(jnp.where(moved, OWN, kept), 128)
        first = jnp.where(ci == 0, OWN * cc, OWN * cc - 256)
        qs = _al(jnp.where(moved, jnp.where(ci == 0, 1024 + 128 * cc, 256), first + kept), 128)
        for n in range(8):
            at = slice(256 * n, 256 * n + 256)
            t = _dot(qo[pl.ds(qs, 128), :], wqo[:, at], 1, 0) + _dot(ox[pl.ds(slot, 128), :], wkv[:, at], 1, 0)
            xs[pl.ds(slot, 128), at] = (xs[pl.ds(slot, 128), at].astype(jnp.float32) + t).astype(jnp.bfloat16)

        @pl.when(moved)
        def _():
            send_y(cc).start()

    lax.fori_loop(0, jnp.where(ci == 0, 5, 3), out, None)

    send_a.wait_send()

    @pl.when(ci == 0)
    def _():
        for c in range(4):
            send_far(c).wait_send()
        send_at.wait_send()
        send_o(0, 128, OWN, 8).wait_send()
        send_o(0, 256, 0, 9).wait_send()
        send_o(0, 256, 0, 10).wait_send()
        send_y(cc).wait_send()

    @pl.when(ci == 1)
    def _():
        for c in range(4):
            relay(c).wait_send()

    @pl.when(me == 2)
    def _():
        send_o(0, 128, 128, 9).wait_send()
        send_o(0, 256, 256, 10).wait_send()
        send_xt(0).wait_send()
        send_xt(1).wait_send()
        send_y(0).wait_send()
        send_y(0).wait_recv()
        send_y(1).wait_recv()

    @pl.when(me == 3)
    def _():
        send_o(0, 256, 256, 9).wait_send()
        send_o(0, 128, OWN, 8).wait_send()
        send_xm.wait_send()
        send_y(0).wait_recv()


def _tables():
    freq = THETA ** (-np.arange(64) / 64.0)
    sign = np.concatenate([-np.ones(64), np.ones(64)])

    def both(place):
        angle = np.tile(place[:, None] * freq, (1, 2))
        return np.concatenate([np.cos(angle), np.sin(angle) * sign]).astype(np.float32)

    return both(128.0 * np.arange(16)), both(np.arange(128.0))


def solution(mesh):
    hi, lo = _tables()
    any_, vmem = pl.BlockSpec(memory_space=pl.ANY), pl.BlockSpec(memory_space=pltpu.VMEM)
    bf, f32 = jnp.bfloat16, jnp.float32

    def step(x, gain, wq, wk, wv, wo):
        out = pl.pallas_call(
            _kernel,
            out_shape=pltpu.VMEM((OWN + 128, D), bf),
            in_specs=[any_, vmem, vmem, vmem, any_, any_, any_, any_],
            out_specs=vmem,
            scratch_shapes=[
                pltpu.VMEM((2048, D), bf),
                pltpu.VMEM((D, D), bf),
                pltpu.VMEM((D, D), bf),
                pltpu.VMEM((KVH, 2048, HEAD), bf),
                pltpu.VMEM((KVH, HEAD + 16, 2048), bf),
                pltpu.VMEM((1024 + TM, D), bf),
                pltpu.VMEM((OWN + 128, D), bf),
                pltpu.VMEM((3, KVH, 1, COLS), f32),
                pltpu.VMEM((3, KVH, HEAD + 8, COLS), f32),
                pltpu.VMEM((BK, COLS), f32),
                pltpu.VMEM((BK, COLS), f32),
                pltpu.VMEM((2, 1, COLS), f32),
                pltpu.VMEM((2, 1, COLS), f32),
                pltpu.VMEM((2 * BK, BQ), f32),
                pltpu.SemaphoreType.DMA((6,)),
                pltpu.SemaphoreType.DMA((24,)),
                pltpu.SemaphoreType.DMA((24,)),
            ],
            compiler_params=pltpu.CompilerParams(collective_id=0, has_side_effects=True, vmem_limit_bytes=60 * 2**20),
        )(x, gain, jnp.asarray(hi), jnp.asarray(lo), wq, wk, wv, wo)
        return out[:OWN]

    tokens, whole = P(("dp", "sp"), None), P(None, None)
    return jax.shard_map(step, mesh=mesh, in_specs=(tokens, P(None), whole, whole, whole, whole), out_specs=tokens, check_vma=False)
```

```python
import functools

import jax
import jax.numpy as jnp
import numpy as np
from jax import lax
from jax.experimental import pallas as pl
from jax.experimental.pallas import tpu as pltpu
from jax.sharding import PartitionSpec as P

HEAD = 128
THETA = 10000
NEG = -1e30
HIDDEN = 2 * NEG
SEEN = 3e38
ALL, SECOND, FIRST = 0, 256, 512
LOG2E = 1.4426950408889634
E = HEAD**-0.5 * LOG2E
D = 2048
KVH = 8
BQ = 256
NEAR = 1024
BK = 512
COLS = 2 * BQ
OWN = 512
TM = 256
MESH = pl.DeviceIdType.MESH


def _dot(a, b, ca, cb):
    return lax.dot_general(a, b, (((ca,), (cb,)), ((), ())), preferred_element_type=jnp.float32)


def _al(v, n):
    return pl.multiple_of(v, n)


def _kernel(x_ref, gain_ref, hi_ref, lo_ref, wq_ref, wk_ref, wv_ref, wo_ref, xs,
            ab, wkv, wqo, kb, vt, qo, ox, top, mix, sa, sb, ma, mb, vis, loc, snd, rcv):
    me = lax.axis_index("sp")
    ci, cc = lax.div(me, 2), lax.rem(me, 2)
    par = 2 * ci + 1 - cc
    far = 2 * (1 - ci) + cc

    def local(src, dst, i):
        return pltpu.make_async_copy(src, dst, loc.at[i])

    def remote(src, dst, i, to, s=None):
        return pltpu.make_async_remote_copy(src_ref=src, dst_ref=dst, send_sem=snd.at[i if s is None else s], recv_sem=rcv.at[i],
                                            device_id={"sp": to}, device_id_type=MESH)

    get_x = local(x_ref, xs.at[pl.ds(0, OWN)], 0)
    get_wk = local(wk_ref.at[:, pl.ds(_al(cc * NEAR, NEAR), NEAR)], wkv.at[:, pl.ds(0, NEAR)], 1)
    get_wv = local(wv_ref.at[:, pl.ds(_al(cc * NEAR, NEAR), NEAR)], wkv.at[:, pl.ds(NEAR, NEAR)], 2)
    get_wq = local(wq_ref.at[:, pl.ds(_al(cc * D, D), D)], wqo, 3)
    get_wo = local(wo_ref.at[pl.ds(_al(cc * D, D), D)], wqo, 4)
    get_wo2 = local(wo_ref.at[pl.ds(_al((1 - cc) * D, D), D)], wkv, 5)
    get_x.start()
    get_wv.start()
    get_wk.start()

    barrier = pltpu.get_barrier_semaphore()
    for k in range(1, 4):
        pl.semaphore_signal(barrier, inc=1, device_id={"sp": lax.rem(me + k, 4)}, device_id_type=MESH)

    for h in range(KVH):
        vt[h, HEAD:, :] = jnp.ones((16, D), jnp.bfloat16)
        for slot in range(3):
            mix[slot, h] = jnp.zeros((HEAD + 8, COLS), jnp.float32)

    for j in range(4):
        key = lax.broadcasted_iota(jnp.int32, (BQ, BQ), 0) + (BQ * j - BK)
        vis[BQ * j : BQ * j + BQ, :] = jnp.where(key <= lax.broadcasted_iota(jnp.int32, (BQ, BQ), 1), SEEN, HIDDEN)

    get_x.wait()
    pl.semaphore_wait(barrier, 3)

    mine = _al(me * OWN, OWN)
    theirs = _al(par * OWN, OWN)
    send_a = remote(ab.at[pl.ds(mine, OWN)], ab.at[pl.ds(mine, OWN)], 0, par)

    def send_far(c):
        return remote(ab.at[pl.ds(_al(mine + HEAD * c, HEAD), HEAD)], ab.at[pl.ds(_al(BQ * c + HEAD * cc, HEAD), HEAD)], 16 + c, far)

    def relay(c):
        at = pl.ds(_al(BQ * c + HEAD * cc, HEAD), HEAD)
        return remote(ab.at[at], ab.at[at], 20 + c, par)

    def send_xt(k):
        return remote(x_ref.at[pl.ds(HEAD * k, HEAD)], xs.at[pl.ds(OWN, HEAD)], 5, k, 5 + k)

    at_t = pl.ds(_al(NEAR + cc * HEAD, HEAD), HEAD)
    send_at = remote(ab.at[at_t], ab.at[at_t], 7, par)

    def send_o(src, rows, dst, i):
        return remote(qo.at[pl.ds(src, rows)], ox.at[pl.ds(dst, rows)], i, par)

    send_xm = remote(x_ref.at[pl.ds(0, HEAD)], xs.at[pl.ds(OWN, HEAD)], 5, 2)

    def send_y(c):
        return remote(xs.at[pl.ds(OWN, HEAD)], xs.at[pl.ds(_al(HEAD * c, HEAD), HEAD)], 13 + c, jnp.where(ci == 0, 2, 3))

    def norm(ref, src, dst, rows):
        gain = gain_ref[...].astype(jnp.float32).reshape(1, D)

        def some(j, _):
            for k in range(4):
                wide = ref[pl.ds(_al(src + 64 * j + 16 * k, 16), 16), :].astype(jnp.float32)
                scale = lax.rsqrt(jnp.mean(wide * wide, -1, keepdims=True) + 1e-6)
                ab[pl.ds(_al(dst + 64 * j + 16 * k, 16), 16), :] = (wide * scale * gain).astype(jnp.bfloat16)
        lax.fori_loop(0, rows // 64, some, None)

    for c in range(4):
        norm(xs, HEAD * c, mine + HEAD * c, HEAD)

        @pl.when(ci == 0)
        def _():
            send_far(c).start()

    send_a.start()

    @pl.when(me == 2)
    def _():
        send_xt(0).start()
        send_xt(1).start()

    @pl.when(me == 3)
    def _():
        send_xm.start()

    def angles(*places):
        cl, sl = lo_ref[:HEAD, :], lo_ref[HEAD:, :]
        cs, ss = [], []
        for n in places:
            ch, sh = hi_ref[pl.ds(n, 1), :], hi_ref[pl.ds(16 + n, 1), :]
            cs.append(ch * cl - sh * sl)
            ss.append(sh * cl + ch * sl)
        return jnp.concatenate(cs, 0), jnp.concatenate(ss, 0)

    def turned(t, cos, sin):
        t = t.astype(jnp.bfloat16).astype(jnp.float32)
        return (t * cos + pltpu.roll(t, 64, 1) * sin).astype(jnp.bfloat16)

    def kv_step(*runs, halfway=None):
        turns = [angles(*n) for _, *n in runs]
        for n in range(4):
            for (r, *_), (cos, sin) in zip(runs, turns):
                t = _dot(ab[pl.ds(r, BQ), :], wkv[:, NEAR + BQ * n : NEAR + BQ * n + BQ], 1, 0).astype(jnp.bfloat16)
                for k in range(2):
                    vt[2 * n + k, :HEAD, pl.ds(r, BQ)] = t[:, HEAD * k : HEAD * k + HEAD].T
        if halfway:
            halfway()
        for n in range(4):
            for (r, *_), (cos, sin) in zip(runs, turns):
                t = _dot(ab[pl.ds(r, BQ), :], wkv[:, BQ * n : BQ * n + BQ], 1, 0)
                for k in range(2):
                    kb[2 * n + k, pl.ds(r, BQ), :] = turned(t[:, HEAD * k : HEAD * k + HEAD], cos, sin)

    def q_step(r, pos):
        n = lax.div(r, HEAD)
        cos, sin = angles(n, n + 1)
        for n in range(8):
            t = _dot(ab[pl.ds(r, BQ), :], wqo[:, BQ * n : BQ * n + BQ], 1, 0)
            for k in range(2):
                qo[pl.ds(pos, BQ), BQ * n + HEAD * k : BQ * n + HEAD * k + HEAD] = turned(t[:, HEAD * k : HEAD * k + HEAD], cos, sin)

    bufs = (sa, ma), (sb, mb)

    def scores(buf, most, h, qs, at, keys, view=None, k=0):
        q = jnp.concatenate([qo[pl.ds(qs, BQ), BQ * h + HEAD * n : BQ * h + HEAD * n + HEAD] for n in range(2)], 0)
        s = _dot(kb[h, pl.ds(at, keys), :], q, 1, 1)
        if view is not None:
            bound = vis[pl.ds(_al(view, BQ), keys), :]
            s = jnp.minimum(s, jnp.concatenate([bound, bound], 1))
        buf[keys * k : keys * k + keys] = s
        most[k] = s.max(axis=0, keepdims=True)

    def weigh(buf, most, h, slot, at, keys, k=0):
        old = top[slot, h]
        new = jnp.maximum(old, most[k])
        top[slot, h] = new
        p = jnp.exp2((buf[keys * k : keys * k + keys] - new) * E).astype(jnp.bfloat16)
        add = _dot(vt[h, :, pl.ds(at, keys)], p, 1, 0)
        mix[slot, h] = mix[slot, h] * jnp.exp2((old - new) * E) + add[: HEAD + 8]

    def attend(qs, slot, kp, full, part, few, view, begin, end, qs_next, kp_next, view_next):
        def finish(h):
            total = mix[slot, h, HEAD : HEAD + 1, :]
            out = (mix[slot, h, :HEAD, :] * (1 / total)).T.astype(jnp.bfloat16)
            for n in range(2):
                qo[pl.ds(qs, BQ), BQ * h + HEAD * n : BQ * h + HEAD * n + HEAD] = out[BQ * n : BQ * n + BQ]

        @pl.when(begin)
        def _():
            for h in range(KVH):
                top[slot, h] = jnp.full((1, COLS), NEG, jnp.float32)

        def block(j, keys, view_j):
            at = _al(kp + BK * j, BQ)
            last = j == full + part - 1
            view_n = jnp.where(last, view_next, jnp.where((j == full - 1) & (part == 1), view, ALL))
            for h in range(KVH):
                if h < KVH - 1:
                    scores(*bufs[(h + 1) % 2], h + 1, qs, at, keys, view_j)
                else:
                    scores(*bufs[0], 0, _al(jnp.where(last, qs_next, qs), BQ), _al(jnp.where(last, kp_next, at + BK), BQ), BK, view_n)
                weigh(*bufs[h % 2], h, slot, at, keys)

        lax.fori_loop(0, full, lambda j, _: block(j, BK, None), None)

        def few_keys():
            for g in range(KVH // 2):
                more = g < KVH // 2 - 1
                for k in range(2):
                    scores(*bufs[(g + 1) % 2], 2 * g + 2 + k if more else k, qs if more else qs_next, kp if more else kp_next, BQ, k=k)
                for k in range(2):
                    weigh(*bufs[g % 2], 2 * g + k, slot, kp, BQ, k)

        @pl.when(few)
        def _():
            few_keys()

        @pl.when((part == 1) & (view == FIRST))
        def _():
            block(full, BQ, FIRST)

        @pl.when((part == 1) & (view == SECOND))
        def _():
            block(full, BK, SECOND)

        @pl.when(end)
        def _():
            for h in range(KVH):
                finish(h)

    def pass_on(c):
        send_far(c).wait_recv()
        relay(c).start()

    def phase(p, _):
        def kv(j, _):
            @pl.when((p == 0) & (j == 0))
            def _():
                get_wv.wait()

            @pl.when((p == 0) & (j == 1))
            def _():
                send_a.wait_recv()

            @pl.when(p == 1)
            def _():
                relay(0).wait_recv()
                relay(1).wait_recv()

            ra = _al(jnp.where(p == 0, jnp.where(j == 0, me, par) * OWN, 0), OWN)
            na = lax.div(ra, HEAD)
            def halfway():
                @pl.when((p == 0) & (j == 0))
                def _():
                    get_wk.wait()
                    get_wq.start()

            rb = _al(ra + BQ, BQ)
            kv_step((ra, na, jnp.where(p == 0, na + 1, 4)), (rb, jnp.where(p == 0, na + 2, 1), jnp.where(p == 0, na + 3, 5)), halfway=halfway)

        lax.fori_loop(0, jnp.where(p == 0, 2, jnp.where((ci == 1) & (p == 1), 1, 0)), kv, None)

        @pl.when(((ci == 0) & (p == 1)) | ((ci == 1) & (p > 1)))
        def _():
            @pl.when(ci == 0)
            def _():
                send_at.wait_recv()

            @pl.when(ci == 1)
            def _():
                relay(p).wait_recv()

            kv_step((_al(jnp.where(ci == 0, NEAR, BQ * p), BQ), jnp.where(ci == 0, 8, p), jnp.where(ci == 0, 9, 4 + p)))

        @pl.when(p == 1 + 2 * ci)
        def _():
            get_wo2.start()

        def q(j, _):
            @pl.when((p == 0) & (j == 0))
            def _():
                get_wq.wait()

            @pl.when((p == 0) & (ci == 0) & (j == 2))
            def _():
                send_xt(0).wait_recv()
                norm(xs, OWN, NEAR + cc * HEAD, HEAD)
                send_at.start()

            pos = jnp.where(p == 0, BQ * j, NEAR)
            q_step(_al(pos + 1280 * ci, BQ), _al(pos, BQ))

        n_q = jnp.where(p == 0, 4 - ci, jnp.where((p == 1) & (ci == 0), 1, 0))
        lax.fori_loop(0, n_q, q, None)

        @pl.when(p == 1 - ci)
        def _():
            get_wo.start()

        def item(it):
            b = lax.rem(it + 1 - cc, 3)
            t = it - 1
            o = jnp.where(it == 0, NEAR, jnp.where(t < 2, 1 - cc, cc) * OWN + BQ * lax.rem(t + 2, 2))
            qs = jnp.where(ci == 0, o, BQ * b)
            q0 = jnp.where(ci == 0, o, BQ + BQ * b)
            return t, b, _al(qs, BQ), q0

        own_keys = (ci == 0) | (p == 0)
        kp = _al(jnp.where(ci == 0, 0, jnp.where(p == 0, NEAR, jnp.where(p == 1, 0, BQ * p))), BQ)
        n_att = jnp.where(ci == 1, 3, jnp.where(p == 1, 5, 0))

        def last_view(q0):
            return jnp.where(own_keys, jnp.where(lax.rem(q0, 512) == 0, FIRST, SECOND), ALL)

        def blocks(q0):
            return jnp.where(own_keys, lax.div(q0, 512), jnp.where(few, 0, 1))

        def first_view(q0):
            return jnp.where(blocks(q0) == 0, last_view(q0), ALL)

        few = p > 1

        @pl.when((n_att > 0) & few)
        def _():
            for k in range(2):
                scores(sa, ma, k, item(0)[2], kp, BQ, k=k)

        @pl.when((n_att > 0) & jnp.logical_not(few))
        def _():
            _, _, qs, q0 = item(0)
            scores(sa, ma, 0, qs, kp, BK, first_view(q0))

        def att(it, _):
            t, b, qs, q0 = item(it)
            _, _, qs_next, q0_next = item(jnp.minimum(it + 1, n_att - 1))

            @pl.when((ci == 1) & (p == 0) & (it > 0))
            def _():
                pass_on(it - 1)

            @pl.when(((p == 1) | (p == 2)) & (ci == 1) & (it == 2))
            def _():
                pass_on(p + 1)

            attend(qs, jnp.where(ci == 0, 0, b), kp, blocks(q0), jnp.where(own_keys, 1, 0), few, last_view(q0), own_keys, (ci == 0) | (p == 3),
                   qs_next, kp, first_view(q0_next))

            @pl.when((ci == 0) & (it == 0))
            def _():
                send_o(_al(NEAR + HEAD * (1 - cc), HEAD), HEAD, OWN, 8).start()

            @pl.when((ci == 0) & (it > 0) & (it < 3))
            def _():
                send_o(_al(qs, BQ), BQ, _al(BQ * t, BQ), 8 + it).start()

            @pl.when((ci == 1) & (p == 3) & (((cc == 0) & (it == 1)) | ((cc == 1) & (it == 0))))
            def _():
                send_o(qs, BQ, BQ, 10 - cc).start()

            @pl.when((ci == 1) & (p == 3) & (((cc == 0) & (it == 0)) | ((cc == 1) & (it == 1))))
            def _():
                send_o(_al(qs + HEAD * (1 - cc), HEAD), HEAD, _al(HEAD + 384 * cc, HEAD), 9 - cc).start()

        lax.fori_loop(0, n_att, att, None)

    lax.fori_loop(0, 4, phase, None)

    get_wo.wait()
    get_wo2.wait()

    def out(o, _):
        moved = (o == 0) & (me < 3)

        @pl.when((o == 0) & (me != 3))
        def _():
            send_o(0, HEAD, OWN, 8).wait_recv()

        @pl.when(((ci == 0) & (o == 1)) | ((me == 2) & (o == 1)))
        def _():
            send_o(0, BQ, 0, 9).wait_recv()

        @pl.when((me == 3) & (o == 0))
        def _():
            send_o(0, HEAD, HEAD, 9).wait_recv()

        @pl.when(((ci == 0) & (o == 1)) | ((me == 3) & (o == 1)))
        def _():
            send_o(0, BQ, 0, 10).wait_recv()

        @pl.when((me == 2) & (o == 0))
        def _():
            send_xm.wait_recv()

        kept = jnp.where(ci == 0, HEAD * (o - 1), HEAD + HEAD * o)
        slot = _al(jnp.where(moved, OWN, kept), HEAD)
        first = jnp.where(ci == 0, OWN * cc, OWN * cc - BQ)
        qs = _al(jnp.where(moved, jnp.where(ci == 0, NEAR + HEAD * cc, BQ), first + kept), HEAD)
        for n in range(8):
            at = slice(BQ * n, BQ * n + BQ)
            t = _dot(qo[pl.ds(qs, HEAD), :], wqo[:, at], 1, 0) + _dot(ox[pl.ds(slot, HEAD), :], wkv[:, at], 1, 0)
            xs[pl.ds(slot, HEAD), at] = (xs[pl.ds(slot, HEAD), at].astype(jnp.float32) + t).astype(jnp.bfloat16)

        @pl.when(moved)
        def _():
            send_y(cc).start()

    lax.fori_loop(0, jnp.where(ci == 0, 5, 3), out, None)

    send_a.wait_send()

    @pl.when(ci == 0)
    def _():
        for c in range(4):
            send_far(c).wait_send()
        send_at.wait_send()
        send_o(0, HEAD, OWN, 8).wait_send()
        send_o(0, BQ, 0, 9).wait_send()
        send_o(0, BQ, 0, 10).wait_send()
        send_y(cc).wait_send()

    @pl.when(ci == 1)
    def _():
        for c in range(4):
            relay(c).wait_send()

    @pl.when(me == 2)
    def _():
        send_o(0, HEAD, HEAD, 9).wait_send()
        send_o(0, BQ, BQ, 10).wait_send()
        send_xt(0).wait_send()
        send_xt(1).wait_send()
        send_y(0).wait_send()
        send_y(0).wait_recv()
        send_y(1).wait_recv()

    @pl.when(me == 3)
    def _():
        send_o(0, BQ, BQ, 9).wait_send()
        send_o(0, HEAD, OWN, 8).wait_send()
        send_xm.wait_send()
        send_y(0).wait_recv()


def _tables():
    freq = THETA ** (-np.arange(64) / 64.0)
    sign = np.concatenate([-np.ones(64), np.ones(64)])

    def both(place):
        angle = np.tile(place[:, None] * freq, (1, 2))
        return np.concatenate([np.cos(angle), np.sin(angle) * sign]).astype(np.float32)

    return both(128.0 * np.arange(16)), both(np.arange(128.0))


def solution(mesh):
    hi, lo = _tables()
    any_, vmem = pl.BlockSpec(memory_space=pl.ANY), pl.BlockSpec(memory_space=pltpu.VMEM)
    bf, f32 = jnp.bfloat16, jnp.float32

    def step(x, gain, wq, wk, wv, wo):
        out = pl.pallas_call(
            _kernel,
            out_shape=pltpu.VMEM((OWN + 128, D), bf),
            in_specs=[any_, vmem, vmem, vmem, any_, any_, any_, any_],
            out_specs=vmem,
            scratch_shapes=[
                pltpu.VMEM((2048, D), bf),
                pltpu.VMEM((D, D), bf),
                pltpu.VMEM((D, D), bf),
                pltpu.VMEM((KVH, 2048, HEAD), bf),
                pltpu.VMEM((KVH, HEAD + 16, 2048), bf),
                pltpu.VMEM((1024 + TM, D), bf),
                pltpu.VMEM((OWN + 128, D), bf),
                pltpu.VMEM((3, KVH, 1, COLS), f32),
                pltpu.VMEM((3, KVH, HEAD + 8, COLS), f32),
                pltpu.VMEM((BK, COLS), f32),
                pltpu.VMEM((BK, COLS), f32),
                pltpu.VMEM((2, 1, COLS), f32),
                pltpu.VMEM((2, 1, COLS), f32),
                pltpu.VMEM((2 * BK, BQ), f32),
                pltpu.SemaphoreType.DMA((6,)),
                pltpu.SemaphoreType.DMA((24,)),
                pltpu.SemaphoreType.DMA((24,)),
            ],
            compiler_params=pltpu.CompilerParams(collective_id=0, has_side_effects=True, vmem_limit_bytes=60 * 2**20),
        )(x, gain, jnp.asarray(hi), jnp.asarray(lo), wq, wk, wv, wo)
        return out[:OWN]

    tokens, whole = P(("dp", "sp"), None), P(None, None)
    return jax.shard_map(step, mesh=mesh, in_specs=(tokens, P(None), whole, whole, whole, whole), out_specs=tokens, check_vma=False)
```

```python
import functools

import jax
import jax.numpy as jnp
import numpy as np
from jax import lax
from jax.experimental import pallas as pl
from jax.experimental.pallas import tpu as pltpu
from jax.sharding import PartitionSpec as P

HEAD = 128
THETA = 10000
NEG = -1e30
HIDDEN = 2 * NEG
SEEN = 3e38
ALL, SECOND, FIRST = 0, 256, 512
LOG2E = 1.4426950408889634
E = HEAD**-0.5 * LOG2E
D = 2048
KVH = 8
BQ = 256
NEAR = 1024
BK = 512
COLS = 2 * BQ
OWN = 512
TM = 256
MESH = pl.DeviceIdType.MESH


def _dot(a, b, ca, cb):
    return lax.dot_general(a, b, (((ca,), (cb,)), ((), ())), preferred_element_type=jnp.float32)


def _al(v, n):
    return pl.multiple_of(v, n)


def _kernel(x_ref, gain_ref, hi_ref, lo_ref, wq_ref, wk_ref, wv_ref, wo_ref, xs,
            xt, ab, wkv, wqo, kb, vt, qo, ox, top, mix, sa, sb, sc, sd, ma, mb, mc, md, vis, loc, snd, rcv):
    me = lax.axis_index("sp")
    ci, cc = lax.div(me, 2), lax.rem(me, 2)
    par = 2 * ci + 1 - cc
    far = 2 * (1 - ci) + cc

    def local(src, dst, i):
        return pltpu.make_async_copy(src, dst, loc.at[i])

    def remote(src, dst, i, to, s=None):
        return pltpu.make_async_remote_copy(src_ref=src, dst_ref=dst, send_sem=snd.at[i if s is None else s], recv_sem=rcv.at[i],
                                            device_id={"sp": to}, device_id_type=MESH)

    get_x = local(x_ref, xs, 0)
    get_wk = local(wk_ref.at[:, pl.ds(_al(cc * NEAR, NEAR), NEAR)], wkv.at[:, pl.ds(0, NEAR)], 1)
    get_wv = local(wv_ref.at[:, pl.ds(_al(cc * NEAR, NEAR), NEAR)], wkv.at[:, pl.ds(NEAR, NEAR)], 2)
    get_wq = local(wq_ref.at[:, pl.ds(_al(cc * D, D), D)], wqo, 3)
    get_wo = local(wo_ref.at[pl.ds(_al(cc * D, D), D)], wqo, 4)
    get_wo2 = local(wo_ref.at[pl.ds(_al((1 - cc) * D, D), D)], wkv, 5)
    get_x.start()
    get_wv.start()
    get_wk.start()

    barrier = pltpu.get_barrier_semaphore()
    for k in range(1, 4):
        pl.semaphore_signal(barrier, inc=1, device_id={"sp": lax.rem(me + k, 4)}, device_id_type=MESH)

    for h in range(KVH):
        vt[h, HEAD:, :] = jnp.ones((16, D), jnp.bfloat16)
        for slot in range(3):
            mix[slot, h] = jnp.zeros((HEAD + 8, COLS), jnp.float32)

    for j in range(4):
        key = lax.broadcasted_iota(jnp.int32, (BQ, BQ), 0) + (BQ * j - BK)
        vis[BQ * j : BQ * j + BQ, :] = jnp.where(key <= lax.broadcasted_iota(jnp.int32, (BQ, BQ), 1), SEEN, HIDDEN)

    get_x.wait()
    pl.semaphore_wait(barrier, 3)

    mine = _al(me * OWN, OWN)
    theirs = _al(par * OWN, OWN)
    send_a = remote(ab.at[pl.ds(mine, OWN)], ab.at[pl.ds(mine, OWN)], 0, par)

    def send_far(c):
        return remote(ab.at[pl.ds(_al(mine + HEAD * c, HEAD), HEAD)], ab.at[pl.ds(_al(BQ * c + HEAD * cc, HEAD), HEAD)], 16 + c, far)

    def relay(c):
        at = pl.ds(_al(BQ * c + HEAD * cc, HEAD), HEAD)
        return remote(ab.at[at], ab.at[at], 20 + c, par)

    def send_xt(k):
        return remote(x_ref.at[pl.ds(HEAD * k, HEAD)], xt, 5, k, 5 + k)

    at_t = pl.ds(_al(NEAR + cc * HEAD, HEAD), HEAD)
    send_at = remote(ab.at[at_t], ab.at[at_t], 7, par)

    def send_o(src, rows, dst, i):
        return remote(qo.at[pl.ds(src, rows)], ox.at[pl.ds(dst, rows)], i, par)

    send_xm = remote(x_ref.at[pl.ds(0, HEAD)], xt, 5, 2)

    def send_y(c):
        return remote(xt, xs.at[pl.ds(_al(HEAD * c, HEAD), HEAD)], 13 + c, jnp.where(ci == 0, 2, 3))

    def norm(ref, src, dst, rows):
        gain = gain_ref[...].astype(jnp.float32).reshape(1, D)

        def some(j, _):
            for k in range(4):
                wide = ref[pl.ds(_al(src + 64 * j + 16 * k, 16), 16), :].astype(jnp.float32)
                scale = lax.rsqrt(jnp.mean(wide * wide, -1, keepdims=True) + 1e-6)
                ab[pl.ds(_al(dst + 64 * j + 16 * k, 16), 16), :] = (wide * scale * gain).astype(jnp.bfloat16)
        lax.fori_loop(0, rows // 64, some, None)

    for c in range(4):
        norm(xs, HEAD * c, mine + HEAD * c, HEAD)

        @pl.when(ci == 0)
        def _():
            send_far(c).start()

    send_a.start()

    @pl.when(me == 2)
    def _():
        send_xt(0).start()
        send_xt(1).start()

    @pl.when(me == 3)
    def _():
        send_xm.start()

    def angles(*places):
        cl, sl = lo_ref[:HEAD, :], lo_ref[HEAD:, :]
        cs, ss = [], []
        for n in places:
            ch, sh = hi_ref[pl.ds(n, 1), :], hi_ref[pl.ds(16 + n, 1), :]
            cs.append(ch * cl - sh * sl)
            ss.append(sh * cl + ch * sl)
        return jnp.concatenate(cs, 0), jnp.concatenate(ss, 0)

    def turned(t, cos, sin):
        t = t.astype(jnp.bfloat16).astype(jnp.float32)
        return (t * cos + pltpu.roll(t, 64, 1) * sin).astype(jnp.bfloat16)

    def kv_step(*runs, halfway=None):
        turns = [angles(*n) for _, *n in runs]
        for n in range(4):
            for (r, *_), (cos, sin) in zip(runs, turns):
                t = _dot(ab[pl.ds(r, BQ), :], wkv[:, NEAR + BQ * n : NEAR + BQ * n + BQ], 1, 0).astype(jnp.bfloat16)
                for k in range(2):
                    vt[2 * n + k, :HEAD, pl.ds(r, BQ)] = t[:, HEAD * k : HEAD * k + HEAD].T
        if halfway:
            halfway()
        for n in range(4):
            for (r, *_), (cos, sin) in zip(runs, turns):
                t = _dot(ab[pl.ds(r, BQ), :], wkv[:, BQ * n : BQ * n + BQ], 1, 0)
                for k in range(2):
                    kb[2 * n + k, pl.ds(r, BQ), :] = turned(t[:, HEAD * k : HEAD * k + HEAD], cos, sin)

    def q_step(r, pos):
        n = lax.div(r, HEAD)
        cos, sin = angles(n, n + 1)
        for n in range(8):
            t = _dot(ab[pl.ds(r, BQ), :], wqo[:, BQ * n : BQ * n + BQ], 1, 0)
            for k in range(2):
                qo[pl.ds(pos, BQ), BQ * n + HEAD * k : BQ * n + HEAD * k + HEAD] = turned(t[:, HEAD * k : HEAD * k + HEAD], cos, sin)

    bufs = (sa, ma), (sb, mb), (sc, mc), (sd, md)

    def scores(buf, most, h, qs, at, keys, view=None, k=0):
        q = jnp.concatenate([qo[pl.ds(qs, BQ), BQ * h + HEAD * n : BQ * h + HEAD * n + HEAD] for n in range(2)], 0)
        s = _dot(kb[h, pl.ds(at, keys), :], q, 1, 1)
        if view is not None:
            bound = vis[pl.ds(_al(view, BQ), keys), :]
            s = jnp.minimum(s, jnp.concatenate([bound, bound], 1))
        buf[keys * k : keys * k + keys] = s
        most[k] = s.max(axis=0, keepdims=True)

    def weigh(buf, most, h, slot, at, keys, k=0):
        old = top[slot, h]
        new = jnp.maximum(old, most[k])
        top[slot, h] = new
        p = jnp.exp2((buf[keys * k : keys * k + keys] - new) * E).astype(jnp.bfloat16)
        add = _dot(vt[h, :, pl.ds(at, keys)], p, 1, 0)
        mix[slot, h] = mix[slot, h] * jnp.exp2((old - new) * E) + add[: HEAD + 8]

    def attend(qs, slot, kp, full, part, few, view, begin, end, qs_next, kp_next, view_next):
        def finish(h):
            total = mix[slot, h, HEAD : HEAD + 1, :]
            out = (mix[slot, h, :HEAD, :] * (1 / total)).T.astype(jnp.bfloat16)
            for n in range(2):
                qo[pl.ds(qs, BQ), BQ * h + HEAD * n : BQ * h + HEAD * n + HEAD] = out[BQ * n : BQ * n + BQ]

        @pl.when(begin)
        def _():
            for h in range(KVH):
                top[slot, h] = jnp.full((1, COLS), NEG, jnp.float32)

        def block(j, keys, view_j):
            at = _al(kp + BK * j, BQ)
            last = j == full + part - 1
            view_n = jnp.where(last, view_next, jnp.where((j == full - 1) & (part == 1), view, ALL))
            for h in range(KVH):
                if h < KVH - 2:
                    scores(*bufs[(h + 2) % 4], h + 2, qs, at, keys, view_j)
                else:
                    k = h + 2 - KVH
                    scores(*bufs[k], k, _al(jnp.where(last, qs_next, qs), BQ), _al(jnp.where(last, kp_next, at + BK), BQ), BK, view_n)
                weigh(*bufs[h % 4], h, slot, at, keys)

        lax.fori_loop(0, full, lambda j, _: block(j, BK, None), None)

        def few_keys():
            for g in range(KVH // 2):
                more = g < KVH // 2 - 1
                for k in range(2):
                    scores(*bufs[(g + 1) % 2], 2 * g + 2 + k if more else k, qs if more else qs_next, kp if more else kp_next, BQ, k=k)
                for k in range(2):
                    weigh(*bufs[g % 2], 2 * g + k, slot, kp, BQ, k)

        @pl.when(few)
        def _():
            few_keys()

        @pl.when((part == 1) & (view == FIRST))
        def _():
            block(full, BQ, FIRST)

        @pl.when((part == 1) & (view == SECOND))
        def _():
            block(full, BK, SECOND)

        @pl.when(end)
        def _():
            for h in range(KVH):
                finish(h)

    def pass_on(c):
        send_far(c).wait_recv()
        relay(c).start()

    def phase(p, _):
        def kv(j, _):
            @pl.when((p == 0) & (j == 0))
            def _():
                get_wv.wait()

            @pl.when((p == 0) & (j == 1))
            def _():
                send_a.wait_recv()

            @pl.when(p == 1)
            def _():
                relay(0).wait_recv()
                relay(1).wait_recv()

            ra = _al(jnp.where(p == 0, jnp.where(j == 0, me, par) * OWN, 0), OWN)
            na = lax.div(ra, HEAD)
            def halfway():
                @pl.when((p == 0) & (j == 0))
                def _():
                    get_wk.wait()
                    get_wq.start()

            rb = _al(ra + BQ, BQ)
            kv_step((ra, na, jnp.where(p == 0, na + 1, 4)), (rb, jnp.where(p == 0, na + 2, 1), jnp.where(p == 0, na + 3, 5)), halfway=halfway)

        lax.fori_loop(0, jnp.where(p == 0, 2, jnp.where((ci == 1) & (p == 1), 1, 0)), kv, None)

        @pl.when(((ci == 0) & (p == 1)) | ((ci == 1) & (p > 1)))
        def _():
            @pl.when(ci == 0)
            def _():
                send_at.wait_recv()

            @pl.when(ci == 1)
            def _():
                relay(p).wait_recv()

            kv_step((_al(jnp.where(ci == 0, NEAR, BQ * p), BQ), jnp.where(ci == 0, 8, p), jnp.where(ci == 0, 9, 4 + p)))

        @pl.when(p == 1 + 2 * ci)
        def _():
            get_wo2.start()

        def q(j, _):
            @pl.when((p == 0) & (j == 0))
            def _():
                get_wq.wait()

            @pl.when((p == 0) & (ci == 0) & (j == 2))
            def _():
                send_xt(0).wait_recv()
                norm(xt, 0, NEAR + cc * HEAD, HEAD)
                send_at.start()

            pos = jnp.where(p == 0, BQ * j, NEAR)
            q_step(_al(pos + 1280 * ci, BQ), _al(pos, BQ))

        n_q = jnp.where(p == 0, 4 - ci, jnp.where((p == 1) & (ci == 0), 1, 0))
        lax.fori_loop(0, n_q, q, None)

        @pl.when(p == 1 - ci)
        def _():
            get_wo.start()

        def item(it):
            b = lax.rem(it + 1 - cc, 3)
            t = it - 1
            o = jnp.where(it == 0, NEAR, jnp.where(t < 2, 1 - cc, cc) * OWN + BQ * lax.rem(t + 2, 2))
            qs = jnp.where(ci == 0, o, BQ * b)
            q0 = jnp.where(ci == 0, o, BQ + BQ * b)
            return t, b, _al(qs, BQ), q0

        own_keys = (ci == 0) | (p == 0)
        kp = _al(jnp.where(ci == 0, 0, jnp.where(p == 0, NEAR, jnp.where(p == 1, 0, BQ * p))), BQ)
        n_att = jnp.where(ci == 1, 3, jnp.where(p == 1, 5, 0))

        def last_view(q0):
            return jnp.where(own_keys, jnp.where(lax.rem(q0, 512) == 0, FIRST, SECOND), ALL)

        def blocks(q0):
            return jnp.where(own_keys, lax.div(q0, 512), jnp.where(few, 0, 1))

        def first_view(q0):
            return jnp.where(blocks(q0) == 0, last_view(q0), ALL)

        few = p > 1

        @pl.when((n_att > 0) & few)
        def _():
            for k in range(2):
                scores(sa, ma, k, item(0)[2], kp, BQ, k=k)

        @pl.when((n_att > 0) & jnp.logical_not(few))
        def _():
            _, _, qs, q0 = item(0)
            for k in range(2):
                scores(*bufs[k], k, qs, kp, BK, first_view(q0))

        def att(it, _):
            t, b, qs, q0 = item(it)
            _, _, qs_next, q0_next = item(jnp.minimum(it + 1, n_att - 1))

            @pl.when((ci == 1) & (p == 0) & (it > 0))
            def _():
                pass_on(it - 1)

            @pl.when(((p == 1) | (p == 2)) & (ci == 1) & (it == 2))
            def _():
                pass_on(p + 1)

            attend(qs, jnp.where(ci == 0, 0, b), kp, blocks(q0), jnp.where(own_keys, 1, 0), few, last_view(q0), own_keys, (ci == 0) | (p == 3),
                   qs_next, kp, first_view(q0_next))

            @pl.when((ci == 0) & (it == 0))
            def _():
                send_o(_al(NEAR + HEAD * (1 - cc), HEAD), HEAD, OWN, 8).start()

            @pl.when((ci == 0) & (it > 0) & (it < 3))
            def _():
                send_o(_al(qs, BQ), BQ, _al(BQ * t, BQ), 8 + it).start()

            @pl.when((ci == 1) & (p == 3) & (((cc == 0) & (it == 1)) | ((cc == 1) & (it == 0))))
            def _():
                send_o(qs, BQ, BQ, 10 - cc).start()

            @pl.when((ci == 1) & (p == 3) & (((cc == 0) & (it == 0)) | ((cc == 1) & (it == 1))))
            def _():
                send_o(_al(qs + HEAD * (1 - cc), HEAD), HEAD, _al(HEAD + 384 * cc, HEAD), 9 - cc).start()

        lax.fori_loop(0, n_att, att, None)

    lax.fori_loop(0, 4, phase, None)

    get_wo.wait()
    get_wo2.wait()

    def out(o, _):
        moved = (o == 0) & (me < 3)

        @pl.when((o == 0) & (me != 3))
        def _():
            send_o(0, HEAD, OWN, 8).wait_recv()

        @pl.when(((ci == 0) & (o == 1)) | ((me == 2) & (o == 1)))
        def _():
            send_o(0, BQ, 0, 9).wait_recv()

        @pl.when((me == 3) & (o == 0))
        def _():
            send_o(0, HEAD, HEAD, 9).wait_recv()

        @pl.when(((ci == 0) & (o == 1)) | ((me == 3) & (o == 1)))
        def _():
            send_o(0, BQ, 0, 10).wait_recv()

        @pl.when((me == 2) & (o == 0))
        def _():
            send_xm.wait_recv()

        kept = jnp.where(ci == 0, HEAD * (o - 1), HEAD + HEAD * o)
        slot = _al(jnp.where(moved, OWN, kept), HEAD)
        first = jnp.where(ci == 0, OWN * cc, OWN * cc - BQ)
        qs = _al(jnp.where(moved, jnp.where(ci == 0, NEAR + HEAD * cc, BQ), first + kept), HEAD)
        def project(ref, row):
            for n in range(8):
                at = slice(BQ * n, BQ * n + BQ)
                t = _dot(qo[pl.ds(qs, HEAD), :], wqo[:, at], 1, 0) + _dot(ox[pl.ds(slot, HEAD), :], wkv[:, at], 1, 0)
                ref[pl.ds(row, HEAD), at] = (ref[pl.ds(row, HEAD), at].astype(jnp.float32) + t).astype(jnp.bfloat16)

        @pl.when(moved)
        def _():
            project(xt, 0)
            send_y(cc).start()

        @pl.when(jnp.logical_not(moved))
        def _():
            project(xs, slot)

    lax.fori_loop(0, jnp.where(ci == 0, 5, 3), out, None)

    send_a.wait_send()

    @pl.when(ci == 0)
    def _():
        for c in range(4):
            send_far(c).wait_send()
        send_at.wait_send()
        send_o(0, HEAD, OWN, 8).wait_send()
        send_o(0, BQ, 0, 9).wait_send()
        send_o(0, BQ, 0, 10).wait_send()
        send_y(cc).wait_send()

    @pl.when(ci == 1)
    def _():
        for c in range(4):
            relay(c).wait_send()

    @pl.when(me == 2)
    def _():
        send_o(0, HEAD, HEAD, 9).wait_send()
        send_o(0, BQ, BQ, 10).wait_send()
        send_xt(0).wait_send()
        send_xt(1).wait_send()
        send_y(0).wait_send()
        send_y(0).wait_recv()
        send_y(1).wait_recv()

    @pl.when(me == 3)
    def _():
        send_o(0, BQ, BQ, 9).wait_send()
        send_o(0, HEAD, OWN, 8).wait_send()
        send_xm.wait_send()
        send_y(0).wait_recv()


def _tables():
    freq = THETA ** (-np.arange(64) / 64.0)
    sign = np.concatenate([-np.ones(64), np.ones(64)])

    def both(place):
        angle = np.tile(place[:, None] * freq, (1, 2))
        return np.concatenate([np.cos(angle), np.sin(angle) * sign]).astype(np.float32)

    return both(128.0 * np.arange(16)), both(np.arange(128.0))


def solution(mesh):
    hi, lo = _tables()
    any_, vmem = pl.BlockSpec(memory_space=pl.ANY), pl.BlockSpec(memory_space=pltpu.VMEM)
    bf, f32 = jnp.bfloat16, jnp.float32

    def step(x, gain, wq, wk, wv, wo):
        return pl.pallas_call(
            _kernel,
            out_shape=pltpu.VMEM((OWN, D), bf),
            in_specs=[any_, vmem, vmem, vmem, any_, any_, any_, any_],
            out_specs=vmem,
            scratch_shapes=[
                pltpu.VMEM((128, D), bf),
                pltpu.VMEM((2048, D), bf),
                pltpu.VMEM((D, D), bf),
                pltpu.VMEM((D, D), bf),
                pltpu.VMEM((KVH, 2048, HEAD), bf),
                pltpu.VMEM((KVH, HEAD + 16, 2048), bf),
                pltpu.VMEM((1024 + TM, D), bf),
                pltpu.VMEM((OWN + 128, D), bf),
                pltpu.VMEM((3, KVH, 1, COLS), f32),
                pltpu.VMEM((3, KVH, HEAD + 8, COLS), f32),
                pltpu.VMEM((BK, COLS), f32),
                pltpu.VMEM((BK, COLS), f32),
                pltpu.VMEM((BK, COLS), f32),
                pltpu.VMEM((BK, COLS), f32),
                pltpu.VMEM((2, 1, COLS), f32),
                pltpu.VMEM((2, 1, COLS), f32),
                pltpu.VMEM((2, 1, COLS), f32),
                pltpu.VMEM((2, 1, COLS), f32),
                pltpu.VMEM((2 * BK, BQ), f32),
                pltpu.SemaphoreType.DMA((6,)),
                pltpu.SemaphoreType.DMA((24,)),
                pltpu.SemaphoreType.DMA((24,)),
            ],
            compiler_params=pltpu.CompilerParams(collective_id=0, has_side_effects=True, vmem_limit_bytes=60 * 2**20),
        )(x, gain, jnp.asarray(hi), jnp.asarray(lo), wq, wk, wv, wo)

    tokens, whole = P(("dp", "sp"), None), P(None, None)
    return jax.shard_map(step, mesh=mesh, in_specs=(tokens, P(None), whole, whole, whole, whole), out_specs=tokens, check_vma=False)
```
